256 devices in a mesh: seq: 32 (over y, z), head: 8 (over x, core).
Axes of the slice: x: 4, y: 4, z: 8, core: 2. Of those that a mesh axis runs over, the one named last changes fastest.
Arguments:
- tokens: bfloat16 [12288, 4096], P('seq', 'head'), may hold values from -6 to 6
- norm_gain: float32 [4096], replicated, may hold values from 0.25 to 1.75
- w_in: bfloat16 [4096, 8, 2304], P('seq', 'head'), may hold values from -0.09375 to 0.09375
- w_dt: bfloat16 [4096, 128], P('seq', 'head'), may hold values from -0.09375 to 0.09375
- dt_bias: float32 [128], P('head'), may hold values from -3 to -1
- a_log: float32 [128], P('head'), may hold values from -11 to -1
- d_skip: float32 [128], P('head'), may hold values from 0.5 to 1.5
- conv_w: float32 [4, 8, 1280], P(None, 'head'), may hold values from -0.5 to 0.5
- conv_b: float32 [8, 1280], P('head'), may hold values from -0.5 to 0.5
- gate_gain: float32 [8, 1024], P('head'), may hold values from 0.25 to 1.75
- w_out: bfloat16 [8, 1024, 4096], P('head'), may hold values from -0.09375 to 0.09375
Outputs:
- mixed: bfloat16 [12288, 4096], P('seq', 'head')
The draws below stay inside these ranges and needn't reach their ends.
All inputs are finite; a program needn't handle non-finite values.
Results may differ from the reference program's by a relative error of at most 0.018.
Values may be sent and summed in bfloat16 or wider, within the bound.
A program may use at most 128 MiB of HBM per device.

```python
import jax
import jax.numpy as jnp
from jax import lax

D = 4096
HEADS = 128
G = 8
P_SIZE = 64
N = 128
KERNEL = 4
STRETCH = 128
TOKENS = 12288
HG = 16


def draw_a_log(key, part):
    chooser, levels = jax.random.split(jax.random.fold_in(key, 17))
    slow_share = 0.5
    is_slow = jax.random.uniform(chooser, (HEADS,), jnp.float32) < slow_share
    position = jax.random.uniform(levels, (HEADS,), jnp.float32)
    low_slow = jnp.log(1.0 / TOKENS)
    high_slow = jnp.log(4.0 / TOKENS)
    low_fast = jnp.log(0.05)
    high_fast = jnp.log(0.2)
    slow_value = low_slow + position * (high_slow - low_slow)
    fast_value = low_fast + position * (high_fast - low_fast)
    return jnp.where(is_slow, slow_value, fast_value).astype(jnp.float32)


def with_spikes(drawn, key, source, target, parts, factor):
    def block_of(axis_at):
        return (jnp.arange(drawn.shape[axis_at]) // (drawn.shape[axis_at] // parts)).reshape((-1,) + (1,) * (drawn.ndim - 1 - axis_at))

    first = jax.random.permutation(key, parts)[block_of(target)]
    other_side = (block_of(target) + parts // 2) % parts
    return jnp.where((block_of(source) == first) | (block_of(source) == other_side), factor * drawn, drawn)


def block_levels(key, dims, cuts, smallest, largest):
    def one(axis_at, blocks):
        draws = jax.random.uniform(jax.random.fold_in(jax.random.fold_in(key, 6), axis_at), (blocks,), jnp.float32, smallest / len(cuts), largest / len(cuts))
        return jnp.repeat(jnp.exp(draws), dims[axis_at] // blocks).reshape((-1,) + (1,) * (len(dims) - axis_at - 1))

    loudness = one(*cuts[0])
    for cut in cuts[1:]:
        loudness = loudness * one(*cut)
    return loudness


def normal_values(own_key, dims, spread, most, shards=(), kind=jnp.bfloat16):
    factor_of = block_levels(own_key, dims, shards, -0.22, 0.18) if shards else 1.0
    values = jax.random.normal(own_key, dims, jnp.float32) * spread * factor_of
    return jnp.minimum(jnp.maximum(values, -most), most).astype(kind)


def bell_draw_with(rng, shape, scale, bound, cuts, heavy, held_as=jnp.bfloat16):
    result = scale * jax.random.normal(rng, shape, jnp.float32)
    if cuts:
        result = result * block_levels(rng, shape, cuts, -0.22, 0.18)
    return jnp.clip(with_spikes(result, jax.random.fold_in(rng, 3), *heavy), -bound, bound).astype(held_as)


def setup_inputs(seed: int = 0) -> dict:
    key_list = jax.random.split(jax.random.key(seed), 12)
    tokens = normal_values(key_list[0], (TOKENS, D), 1.0, 6.0, ((0, 32), (1, 8)))
    norm_gain = jnp.clip(1.0 + 0.15 * jax.random.normal(key_list[1], (D,), jnp.float32), 0.25, 1.75)
    w_in = normal_values(key_list[2], (D, G, 2 * HG * P_SIZE + 2 * N), D ** -0.5, 0.09375, ((0, 32), (1, 8)))
    w_dt = normal_values(key_list[3], (D, HEADS), D ** -0.5, 0.09375, ((0, 32), (1, 8)))
    dt_bias = jnp.clip(-3.0 + 2.0 * jax.random.uniform(key_list[4], (HEADS,), jnp.float32) ** block_levels(key_list[4], (HEADS,), ((0, 8),), -0.2, 0.2), -3.0, -1.0)
    a_log = draw_a_log(jax.random.fold_in(key_list[11], 71), 0)
    d_skip = jnp.clip(0.5 + 1.0 * jax.random.uniform(key_list[6], (HEADS,), jnp.float32) ** block_levels(key_list[6], (HEADS,), ((0, 8),), -0.2, 0.2), 0.5, 1.5)
    conv_w = jnp.clip(jax.random.uniform(key_list[7], (KERNEL, G, HG * P_SIZE + 2 * N), jnp.float32, -0.5, 0.5) * block_levels(key_list[7], (KERNEL, G, HG * P_SIZE + 2 * N), ((1, 8),), -0.4, 0.0), -0.5, 0.5)
    conv_b = jnp.clip(jax.random.uniform(key_list[8], (G, HG * P_SIZE + 2 * N), jnp.float32, -0.5, 0.5) * block_levels(key_list[8], (G, HG * P_SIZE + 2 * N), ((0, 8),), -0.4, 0.0), -0.5, 0.5)
    gate_gain = jnp.clip(1.0 + 0.15 * jax.random.normal(key_list[9], (G, HG * P_SIZE), jnp.float32), 0.25, 1.75)
    w_out = bell_draw_with(key_list[10], (G, HG * P_SIZE, D), (HEADS * P_SIZE) ** -0.5, 0.09375, ((0, 8),), (0, 2, 8, 2.0))
    return {"tokens": tokens, "norm_gain": norm_gain, "w_in": w_in, "w_dt": w_dt, "dt_bias": dt_bias, "a_log": a_log, "d_skip": d_skip, "conv_w": conv_w, "conv_b": conv_b, "gate_gain": gate_gain, "w_out": w_out}


EPS = 1e-05
HIGHEST = lax.Precision.HIGHEST

def normalize(values, gain):
    squares = lax.optimization_barrier(jnp.mean(values * values, axis=-1, keepdims=True))
    return values * lax.rsqrt(squares + EPS) * gain

def state_block(inputs, step_size, log_decay, in_map, out_map, block_len):
    length = inputs.shape[0]
    stretch_count = length // block_len
    head_count = inputs.shape[1]
    head_size = inputs.shape[2]
    state_size = in_map.shape[1]
    shaped = (inputs.reshape(stretch_count, block_len, head_count, head_size), step_size.reshape(stretch_count, block_len, head_count), log_decay.reshape(stretch_count, block_len, head_count), in_map.reshape(stretch_count, block_len, state_size), out_map.reshape(stretch_count, block_len, state_size))
    causal = jnp.arange(block_len)[:, None] >= jnp.arange(block_len)[None, :]

    def advance(state_now, pieces):
        stretch_in, stretch_step, stretch_log, stretch_b, stretch_c = pieces
        cumulative = jnp.cumsum(stretch_log, axis=0)
        gap_log = cumulative[:, None, :] - cumulative[None, :, :]
        decays = jnp.where(causal[:, :, None], jnp.exp(jnp.where(causal[:, :, None], gap_log, 0.0)), 0.0)
        scores = jnp.dot(stretch_c, stretch_b.T, preferred_element_type=jnp.float32)
        wide_c = stretch_c.astype(jnp.float32)
        wide_b = stretch_b.astype(jnp.float32)
        weights = scores[:, :, None] * decays * stretch_step[None, :, :]
        within = jnp.einsum('ijh,jhp->ihp', weights, stretch_in, precision=HIGHEST)
        across = jnp.exp(cumulative)[:, :, None] * jnp.einsum('in,hpn->ihp', wide_c, state_now, precision=HIGHEST)
        to_end = jnp.exp(cumulative[-1][None, :] - cumulative) * stretch_step
        fresh_state = jnp.einsum('jh,jhp,jn->hpn', to_end, stretch_in, wide_b, precision=HIGHEST)
        state_next = jnp.exp(cumulative[-1])[:, None, None] * state_now + fresh_state
        return (state_next, within + across)
    start_state = jnp.zeros((head_count, head_size, state_size), jnp.float32)
    final, outputs = lax.scan(advance, start_state, shaped)
    return (outputs.reshape(length, head_count, head_size), final)

def reference(tokens, norm_gain, w_in, w_dt, dt_bias, a_log, d_skip, conv_w, conv_b, gate_gain, w_out):
    group_width = HG * P_SIZE
    normed = normalize(tokens.astype(jnp.float32), norm_gain).astype(jnp.bfloat16)
    step_all = jax.nn.softplus(jnp.dot(normed, w_dt, preferred_element_type=jnp.float32) + dt_bias)
    rates = jnp.exp(a_log)

    def group_step(totals, group_index):
        weight = lax.dynamic_index_in_dim(w_in, group_index, 1, keepdims=False)
        projected = lax.optimization_barrier(jnp.dot(normed, weight, preferred_element_type=jnp.float32).astype(jnp.bfloat16))
        gate_raw = projected[:, :group_width].astype(jnp.float32)
        channels = projected[:, group_width:].astype(jnp.float32)
        taps = lax.dynamic_index_in_dim(conv_w, group_index, 1, keepdims=False)
        bias_row = lax.dynamic_index_in_dim(conv_b, group_index, 0, keepdims=False)
        padded = jnp.concatenate([jnp.zeros((KERNEL - 1, channels.shape[1]), jnp.float32), channels], axis=0)
        summed = bias_row[None, :]
        for offset in range(KERNEL):
            summed = summed + taps[offset][None, :] * padded[offset:offset + TOKENS]
        narrow = lax.optimization_barrier(jax.nn.silu(summed).astype(jnp.bfloat16))
        convolved = narrow.astype(jnp.float32)
        inputs = convolved[:, :group_width].reshape(TOKENS, HG, P_SIZE)
        in_map = narrow[:, group_width:group_width + N]
        out_map = narrow[:, group_width + N:]
        first = (group_index * HG).astype(jnp.int32)
        step_size = lax.dynamic_slice_in_dim(step_all, first, HG, 1)
        log_decay = -lax.dynamic_slice_in_dim(rates, first, HG, 0)[None, :] * step_size
        skip_row = lax.dynamic_slice_in_dim(d_skip, first, HG, 0)
        outputs, final = state_block(inputs, step_size, log_decay, in_map, out_map, STRETCH)
        outputs = outputs + skip_row[None, :, None] * inputs
        gated = outputs.reshape(TOKENS, group_width) * jax.nn.silu(gate_raw)
        gain_row = lax.dynamic_index_in_dim(gate_gain, group_index, 0, keepdims=False)
        normed_out = normalize(gated, gain_row).astype(jnp.bfloat16)
        out_rows = lax.dynamic_index_in_dim(w_out, group_index, 0, keepdims=False)
        return (totals + jnp.dot(normed_out, out_rows, preferred_element_type=jnp.float32), None)
    totals, unused = lax.scan(group_step, jnp.zeros((TOKENS, D), jnp.float32), jnp.arange(G, dtype=jnp.int32))
    return totals.astype(jnp.bfloat16)
```

```python
import heapq
import itertools

import jax
import jax.numpy as jnp
from jax import lax
from jax.experimental import pallas as pl
from jax.experimental.pallas import tpu as pltpu
from jax.sharding import PartitionSpec as P

EPS = 1e-05
HIGHEST = lax.Precision.HIGHEST
MESH = pl.DeviceIdType.MESH
F32 = jnp.float32
BF16 = jnp.bfloat16

NY, NZ, NX = 4, 8, 4
ROWS = 384
DB = 512
HB = 8
SUB = 128
CC = 1280
GC = 1024
YZ_ROWS = 48
NH = 16
CHUNKS = 3


def children(stream, dy, dz):
    along_z, flip = stream in (0, 2), stream >= 2
    out = []
    if along_z:
        up, down = (3, 4) if flip else (4, 3)
        if dy == 0:
            if 0 <= dz < up:
                out.append((0, dz + 1, "z+"))
            if 0 <= -dz < down:
                out.append((0, dz - 1, "z-"))
            out.append((1, dz, "y+"))
            out.append((-1, dz, "y-"))
        far = 1 if (dz % 2 == 0) != flip else -1
        if dy == far:
            out.append((2 * far, dz, "y+" if far > 0 else "y-"))
    else:
        far = -1 if flip else 1
        if dz == 0:
            if dy == 0:
                out += [(1, 0, "y+"), (-1, 0, "y-")]
            if dy == far:
                out.append((2 * far, 0, "y+" if far > 0 else "y-"))
        up, down = (4, 3) if (dy % 2 == 0) != flip else (3, 4)
        if 0 <= dz < up:
            out.append((dy, dz + 1, "z+"))
        if 0 <= -dz < down:
            out.append((dy, dz - 1, "z-"))
    return out


def arrival_order(late):
    sizes = [(SUB - YZ_ROWS) * CC, YZ_ROWS * CC, (SUB - YZ_ROWS) * GC, YZ_ROWS * GC]
    free = {d: 0.0 for d in ("y+", "y-", "z+", "z-")}
    events, order, tick = [], [], itertools.count()

    def issue(t, stream, dy, dz):
        for a, b, d in children(stream, dy, dz):
            end = max(t, free[d]) + sizes[stream] / 21600.0
            free[d] = end
            heapq.heappush(events, (end + 2.0, next(tick), stream, a, b))

    issue(0.0, 0, 0, 0)
    issue(0.0, 1, 0, 0)
    while events:
        t, _, stream, a, b = heapq.heappop(events)
        order.append((stream, a, b))
        issue(t, stream, a, b)
        if len(order) == late:
            issue(t, 2, 0, 0)
            issue(t, 3, 0, 0)
    return order


LATE = 54
ORDER = arrival_order(LATE)
LAST_C = max(i for i, item in enumerate(ORDER) if item[0] < 2) + 1


def number(dy, dz):
    return (dy % NY) * NZ + dz % NZ


def softplus(v):
    return jnp.maximum(v, 0.0) + jnp.log1p(jnp.exp(-jnp.abs(v)))


def silu(v):
    return v / (1.0 + jnp.exp(-v))


def dot_nt(a, b):
    return lax.dot_general(a, b, (((1,), (1,)), ((), ())), preferred_element_type=F32)


def dot_tn(a, b):
    return lax.dot_general(a, b, (((0,), (0,)), ((), ())), preferred_element_type=F32)


def kernel(
    tok_in, w_in, w_dt, w_out, norm_gain, dt_bias, a_log, d_skip, conv_w, conv_b, gate_gain,
    out_ref,
    tok, xn, wc, wg, wd, wo, chf, halo_out, halo_in, cv, ybuf, tt, ct, fs,
    e_out, d_out, e_in, d_in, pre, row_out, rowd_out, row_in, rowd_in, back_out, sin,
    no, sib_out, sib_in, part, far_out, far_in, near_out, near_in,
    load_sem, w_send, w_recv, t_send, t_recv, h_send, h_recv,
    s_send, s_recv, r_send, r_recv, b_send, b_recv, o_send, o_recv, x_send, x_recv,
):
    s = lax.axis_index("seq")
    hd = lax.axis_index("head")
    y, z = lax.div(s, NZ), lax.rem(s, NZ)
    x, c = lax.div(hd, 2), lax.rem(hd, 2)

    def at_yz(dy, dz):
        return lax.rem(y + dy + 2 * NY, NY) * NZ + lax.rem(z + dz + 2 * NZ, NZ)

    def head_of(dx, core):
        return lax.rem(x + dx + NX, NX) * 2 + core

    sibling = (s, x * 2 + (1 - c))
    plus, minus = (s, head_of(1, c)), (s, head_of(-1, c))
    follow = (lax.rem(s + 1, NY * NZ), hd)
    ahead = (lax.rem(s + NY * NZ - 1, NY * NZ), hd)
    target = {
        "y+": (at_yz(1, 0), hd), "y-": (at_yz(-1, 0), hd),
        "z+": (at_yz(0, 1), hd), "z-": (at_yz(0, -1), hd),
    }
    z_peers = [(at_yz(0, k), hd) for k in range(1, NZ)]
    y_peers = [(at_yz(k, 0), hd) for k in range(1, NY)]
    sent = []

    def remote(src, dst, send, recv, where):
        return pltpu.make_async_remote_copy(
            src_ref=src, dst_ref=dst, send_sem=send, recv_sem=recv, device_id=where, device_id_type=MESH
        )

    def push(src, dst, send, recv, where):
        copy = remote(src, dst, send, recv, where)
        copy.start()
        sent.append(copy)

    def arrived(ref, recv):
        remote(ref, ref, recv, recv, sibling).wait_recv()

    own_rows = pl.ds(pl.multiple_of(s * SUB, SUB), SUB)
    loads = [
        pltpu.make_async_copy(tok_in, tok.at[hd], load_sem.at[0]),
        pltpu.make_async_copy(w_in.at[:, pl.ds(GC, CC)], wc.at[own_rows, :], load_sem.at[1]),
        pltpu.make_async_copy(w_dt, wd.at[:, own_rows], load_sem.at[2]),
        pltpu.make_async_copy(w_in.at[:, pl.ds(0, GC)], wg.at[own_rows, :], load_sem.at[3]),
        pltpu.make_async_copy(w_out, wo, load_sem.at[4]),
    ]
    for copy in loads:
        copy.start()

    barrier = pltpu.get_barrier_semaphore()
    peers = z_peers + y_peers + [plus, minus, sibling, follow, ahead]
    for peer in peers:
        pl.semaphore_signal(barrier, inc=1, device_id=peer, device_id_type=MESH)
    pl.semaphore_wait(barrier, len(peers))

    def block(stream, slot):
        base = slot * SUB
        held = wc if stream < 2 else wg
        if stream in (0, 2):
            return held.at[pl.ds(pl.multiple_of(base + YZ_ROWS, 16), SUB - YZ_ROWS), :]
        return held.at[pl.ds(pl.multiple_of(base, 16), YZ_ROWS), :]

    def dt_block(slot):
        return wd.at[:, pl.ds(pl.multiple_of(slot * SUB, SUB), SUB)]

    def spread(stream, dy, dz):
        slot = at_yz(-dy, -dz)
        for a, b, d in children(stream, dy, dz):
            k = number(a, b)
            piece = block(stream, slot)
            push(piece, piece, w_send.at[stream, k], w_recv.at[stream, k], target[d])
            if stream == 0:
                piece = dt_block(slot)
                push(piece, piece, w_send.at[4, k], w_recv.at[4, k], target[d])

    state = {"at": 0}

    def pump(count, stop=len(ORDER)):
        for _ in range(count):
            if state["at"] >= stop:
                return
            stream, dy, dz = ORDER[state["at"]]
            state["at"] += 1
            slot, k = at_yz(-dy, -dz), number(dy, dz)
            arrived(block(stream, slot), w_recv.at[stream, k])
            if stream == 0:
                arrived(dt_block(slot), w_recv.at[4, k])
            spread(stream, dy, dz)
            if state["at"] == LATE:
                spread(2, 0, 0)
                spread(3, 0, 0)

    loads[1].wait()
    loads[2].wait()
    spread(0, 0, 0)
    spread(1, 0, 0)
    loads[0].wait()

    half = [pl.ds(0, ROWS // 2), pl.ds(ROWS // 2, ROWS // 2)]

    def tok_piece(dx, core, k):
        return tok.at[head_of(dx, core), half[k], :]

    mine = [tok_piece(0, c, 0), tok_piece(0, c, 1)]
    push(mine[0], mine[0], t_send.at[0], t_recv.at[0], plus)
    push(mine[1], mine[1], t_send.at[3], t_recv.at[3], minus)
    push(mine[1], mine[1], t_send.at[1], t_recv.at[1], plus)
    push(mine[0], mine[0], t_send.at[2], t_recv.at[2], minus)
    push(tok.at[hd], tok.at[hd], t_send.at[6], t_recv.at[6], sibling)

    def relay(index, dx, k, twin, onward=None, onward_index=None):
        piece = tok_piece(dx, c, k)
        arrived(piece, t_recv.at[index])
        if onward is not None:
            push(piece, piece, t_send.at[onward_index], t_recv.at[onward_index], onward)
        push(piece, piece, t_send.at[twin], t_recv.at[twin], sibling)

    loads[3].wait()
    pump(4)
    relay(0, -1, 0, 7, plus, 4)
    relay(3, 1, 1, 10, minus, 5)
    pump(5)
    relay(1, -1, 1, 8)
    relay(2, 1, 0, 9)
    pump(5)
    relay(4, 2, 0, 11)
    relay(5, 2, 1, 12)
    pump(2)
    arrived(tok.at[head_of(0, 1 - c)], t_recv.at[6])
    for index, dx, k in ((7, -1, 0), (8, -1, 1), (9, 1, 0), (10, 1, 1), (11, 2, 0), (12, 2, 1)):
        arrived(tok_piece(dx, 1 - c, k), t_recv.at[index])

    def norm_rows(i, carry):
        rows = pl.ds(pl.multiple_of(i * 32, 32), 32)
        total = jnp.zeros((32, 1), F32)
        for h in range(HB):
            v = tok[h, rows, :].astype(F32)
            total = total + jnp.sum(v * v, axis=1, keepdims=True)
        scale = lax.rsqrt(total / (HB * DB) + EPS)
        for h in range(HB):
            v = tok[h, rows, :].astype(F32)
            xn[h, rows, :] = (v * scale * norm_gain[:, h * DB : (h + 1) * DB]).astype(BF16)
        return carry

    for part_of in range(4):
        lax.fori_loop(part_of * 3, part_of * 3 + 3, norm_rows, 0)
        pump(1)
    pump(len(ORDER), LAST_C)

    def channel_tile(i, carry):
        cols = pl.ds(pl.multiple_of(i * 256, 256), 256)
        total = jnp.zeros((ROWS, 256), F32)
        for h in range(HB):
            total = total + jnp.dot(xn[h], wc[h * DB : (h + 1) * DB, cols], preferred_element_type=F32)
        rounded = total.astype(BF16)
        halo_out[:, cols] = rounded[ROWS - 16 :, :]
        chf[8:, cols] = rounded.astype(F32)
        return carry

    for tile in range(5):
        lax.fori_loop(tile, tile + 1, channel_tile, 0)
        pump(1)

    raw = jnp.zeros((NH, ROWS), F32)
    for h in range(HB):
        raw = raw + dot_nt(wd[:, h * DB : (h + 1) * DB], xn[h])

    def column_of(ref):
        wide = jnp.concatenate([ref[...], jnp.zeros((1, 128 - NH), F32)], axis=1)
        return jnp.transpose(jnp.broadcast_to(wide, (128, 128)))[:NH, :1]

    push(halo_out, halo_in, h_send, h_recv, follow)
    step = softplus(raw + column_of(dt_bias))
    decay = -jnp.exp(column_of(a_log)) * step
    row_id = lax.broadcasted_iota(jnp.int32, (128, 128), 0)
    lane_id = lax.broadcasted_iota(jnp.int32, (128, 128), 1)
    upper = jnp.where(row_id <= lane_id, 1.0, 0.0).astype(F32)
    first_half = lane_id < 64
    upper_rows = row_id < 64
    for q in range(CHUNKS):
        span = slice(q * 128, (q + 1) * 128)
        cum = jnp.dot(decay[:, span], upper, precision=HIGHEST, preferred_element_type=F32)
        to_end = jnp.exp(cum[:, 127:128] - cum) * step[:, span]
        ct[q] = cum
        stacked = jnp.concatenate(
            [cum, to_end, step[:, span], jnp.exp(cum), jnp.zeros((64, 128), F32)], axis=0
        )
        tt[q] = jnp.transpose(stacked)
    pump(2)

    arrived(halo_in, h_recv)
    chf[:8, :] = jnp.where(s > 0, halo_in[8:16, :].astype(F32), 0.0)

    def conv_tile(i, carry):
        cols = pl.ds(pl.multiple_of(i * 128, 128), 128)
        for q in range(CHUNKS):
            total = conv_b[:, cols] + jnp.zeros((128, 128), F32)
            for k in range(4):
                total = total + conv_w[k : k + 1, cols] * chf[q * 128 + 5 + k : q * 128 + 133 + k, cols]
            cv[q * 128 : (q + 1) * 128, cols] = silu(total).astype(BF16)
        return carry

    lax.fori_loop(0, 5, conv_tile, 0)
    pump(1)
    lax.fori_loop(5, 10, conv_tile, 0)
    pump(1)

    def pair_cols(table, base, j):
        return jnp.where(
            first_half, table[:, base + 2 * j : base + 2 * j + 1], table[:, base + 2 * j + 1 : base + 2 * j + 2]
        )

    def pair_rows(row, j):
        return jnp.where(upper_rows, jnp.exp(row[:, 2 * j : 2 * j + 1]), jnp.exp(row[:, 2 * j + 1 : 2 * j + 2]))

    for q in range(CHUNKS):
        span = slice(q * 128, (q + 1) * 128)
        b_map, c_map = cv[span, 1024:1152], cv[span, 1152:1280]
        scores = jnp.where(row_id >= lane_id, dot_nt(c_map, b_map), 0.0)
        table = tt[q]
        for j in range(8):
            cols = slice(j * 128, (j + 1) * 128)
            v = cv[span, cols].astype(F32)
            stepped = v * pair_cols(table, 32, j)
            values = jnp.concatenate(
                [jnp.where(first_half, stepped, 0.0), jnp.where(first_half, 0.0, stepped)], axis=0
            ).astype(BF16)
            weights = []
            for h in (2 * j, 2 * j + 1):
                gap = jnp.minimum(table[:, h : h + 1] - ct[q, h : h + 1, :], 0.0)
                weights.append((scores * jnp.exp(gap)).astype(BF16))
            inner = jnp.dot(jnp.concatenate(weights, axis=1), values, preferred_element_type=F32)
            skip = jnp.where(first_half[:1], d_skip[:, 2 * j : 2 * j + 1], d_skip[:, 2 * j + 1 : 2 * j + 2])
            ybuf[span, cols] = inner + skip * v
            fs[q, cols, :] = dot_tn((v * pair_cols(table, 16, j)).astype(BF16), b_map)
            if j % 2 == 1:
                pump(1)

    ends = [tt[q, 127:128, :] for q in range(CHUNKS)]
    for j in range(8):
        cols = slice(j * 128, (j + 1) * 128)
        total = fs[1, cols, :] + pair_rows(ends[1], j) * fs[0, cols, :]
        total = fs[2, cols, :] + pair_rows(ends[2], j) * total
        e_out[j] = total.astype(BF16)
    d_out[...] = jnp.broadcast_to(ends[0] + ends[1] + ends[2], (8, 128))
    pump(1)
    for k in range(1, NZ):
        peer = lax.rem(z + k, NZ)
        push(e_out.at[peer], e_in.at[z], s_send.at[0, k], s_recv.at[0, k], z_peers[k - 1])
        push(d_out, d_in.at[z], s_send.at[1, k], s_recv.at[1, k], z_peers[k - 1])
    e_in[z] = e_out[z]
    d_in[z] = d_out[...]
    pump(5)
    for k in range(1, NZ):
        source = lax.rem(z + NZ - k, NZ)
        arrived(e_in.at[source], s_recv.at[0, k])
        arrived(d_in.at[source], s_recv.at[1, k])

    lane_row = lax.broadcasted_iota(jnp.int32, (1, 128), 1)

    def pick(row, lane):
        return jnp.sum(jnp.where(lane_row == lane, row, 0.0), axis=1, keepdims=True)

    def factor(pair):
        return jnp.where(upper_rows[:, :1], jnp.exp(pair[0]), jnp.exp(pair[1]))

    running = jnp.zeros((128, 128), F32)
    gone = (jnp.zeros((1, 1), F32), jnp.zeros((1, 1), F32))
    before = []
    for k in range(NZ):
        pre[k] = running
        before.append(gone)
        here = d_in[k, :1, :]
        pair = (pick(here, 2 * z), pick(here, 2 * z + 1))
        running = factor(pair) * running + e_in[k].astype(F32)
        gone = (gone[0] + pair[0], gone[1] + pair[1])
    row_out[...] = running.astype(BF16)
    rowd_out[...] = jnp.broadcast_to(jnp.where(lane_row == 0, gone[0], gone[1]), (8, 128))
    pump(1)
    for k in range(1, NY):
        push(row_out, row_in.at[y], r_send.at[0, k], r_recv.at[0, k], y_peers[k - 1])
        push(rowd_out, rowd_in.at[y], r_send.at[1, k], r_recv.at[1, k], y_peers[k - 1])
    row_in[y] = row_out[...]
    rowd_in[y] = rowd_out[...]
    pump(5)
    for k in range(1, NY):
        source = lax.rem(y + NY - k, NY)
        arrived(row_in.at[source], r_recv.at[0, k])
        arrived(rowd_in.at[source], r_recv.at[1, k])
    entering = jnp.zeros((128, 128), F32)
    for k in range(NY):
        here = rowd_in[k, :1, :]
        moved = factor((here[:, 0:1], here[:, 1:2])) * entering + row_in[k].astype(F32)
        entering = jnp.where(k < y, moved, entering)
    for k in range(NZ):
        back_out[k] = (factor(before[k]) * entering + pre[k]).astype(BF16)
    pump(1)
    for k in range(1, NZ):
        peer = lax.rem(z + k, NZ)
        push(back_out.at[peer], sin.at[z], b_send.at[k], b_recv.at[k], z_peers[k - 1])
    sin[z] = back_out[z]
    pump(6)
    for k in range(1, NZ):
        arrived(sin.at[lax.rem(z + NZ - k, NZ)], b_recv.at[k])

    for j in range(8):
        cols = slice(j * 128, (j + 1) * 128)
        held = sin[j].astype(F32)
        for q in range(CHUNKS):
            span = slice(q * 128, (q + 1) * 128)
            across = dot_nt(cv[span, 1152:1280], held.astype(BF16))
            ybuf[span, cols] += pair_cols(tt[q], 48, j) * across
            if q < CHUNKS - 1:
                held = pair_rows(ends[q], j) * held + fs[q, cols, :]
        pump(1)
    pump(len(ORDER))

    def gate_tile(i, total):
        cols = pl.ds(pl.multiple_of(i * 256, 256), 256)
        raw_gate = jnp.zeros((ROWS, 256), F32)
        for h in range(HB):
            raw_gate = raw_gate + jnp.dot(xn[h], wg[h * DB : (h + 1) * DB, cols], preferred_element_type=F32)
        gated = ybuf[:, cols] * silu(raw_gate.astype(BF16).astype(F32))
        ybuf[:, cols] = gated
        return total + jnp.sum(gated * gated, axis=1, keepdims=True)

    total = lax.fori_loop(0, 4, gate_tile, jnp.zeros((ROWS, 1), F32))
    scale = lax.rsqrt(total / GC + EPS)

    def norm_tile(i, carry):
        cols = pl.ds(pl.multiple_of(i * 128, 128), 128)
        no[:, cols] = (ybuf[:, cols] * scale * gate_gain[:, cols]).astype(BF16)
        return carry

    lax.fori_loop(0, 8, norm_tile, 0)
    loads[4].wait()

    def term(dx, core):
        cols = pl.ds(pl.multiple_of(head_of(dx, core) * DB, DB), DB)
        return jnp.dot(no[...], wo[:, cols], preferred_element_type=F32)

    top, low = half
    order = (2, 1, 3, 0)
    for r in order:
        sib_out[r] = term(r, 1 - c).astype(BF16)
        push(sib_out.at[r], sib_in.at[r], o_send.at[r], o_recv.at[r], sibling)
        part[r] = term(r, c)

    def chip_sum(r, rows):
        return part[r, rows, :] + sib_in[r, rows, :].astype(F32)

    arrived(sib_in.at[2], o_recv.at[2])
    far_out[...] = chip_sum(2, slice(None)).astype(BF16)
    push(far_out.at[top, :], far_in.at[0], x_send.at[0], x_recv.at[0], plus)
    push(far_out.at[low, :], far_in.at[1], x_send.at[1], x_recv.at[1], minus)
    arrived(sib_in.at[1], o_recv.at[1])
    near_out[0, low, :] = chip_sum(1, low).astype(BF16)
    push(near_out.at[0, low, :], near_in.at[0, low, :], x_send.at[2], x_recv.at[2], plus)
    arrived(sib_in.at[3], o_recv.at[3])
    near_out[1, top, :] = chip_sum(3, top).astype(BF16)
    push(near_out.at[1, top, :], near_in.at[1, top, :], x_send.at[3], x_recv.at[3], minus)
    arrived(far_in.at[0], x_recv.at[0])
    near_out[0, top, :] = (chip_sum(1, top) + far_in[0].astype(F32)).astype(BF16)
    push(near_out.at[0, top, :], near_in.at[0, top, :], x_send.at[4], x_recv.at[4], plus)
    arrived(far_in.at[1], x_recv.at[1])
    near_out[1, low, :] = (chip_sum(3, low) + far_in[1].astype(F32)).astype(BF16)
    push(near_out.at[1, low, :], near_in.at[1, low, :], x_send.at[5], x_recv.at[5], minus)
    arrived(sib_in.at[0], o_recv.at[0])
    part[0] = chip_sum(0, slice(None))
    arrived(near_in.at[0, low, :], x_recv.at[2])
    arrived(near_in.at[1, top, :], x_recv.at[3])
    arrived(near_in.at[0, top, :], x_recv.at[4])
    arrived(near_in.at[1, low, :], x_recv.at[5])
    out_ref[...] = (part[0] + near_in[0].astype(F32) + near_in[1].astype(F32)).astype(BF16)
    for copy in sent:
        copy.wait_send()


def body(tokens, norm_gain, w_in, w_dt, dt_bias, a_log, d_skip, conv_w, conv_b, gate_gain, w_out):
    any_space = pl.BlockSpec(memory_space=pl.ANY)
    vmem = pl.BlockSpec(memory_space=pltpu.VMEM)
    dma = pltpu.SemaphoreType.DMA

    def buf(*shape, dtype=BF16):
        return pltpu.VMEM(shape, dtype)

    scratch = [
        buf(HB, ROWS, DB), buf(HB, ROWS, DB), buf(4096, CC), buf(4096, GC), buf(NH, 4096), buf(GC, 4096),
        buf(ROWS + 8, CC, dtype=F32), buf(16, CC), buf(16, CC), buf(ROWS, CC), buf(ROWS, GC, dtype=F32),
        buf(CHUNKS, 128, 128, dtype=F32), buf(CHUNKS, NH, 128, dtype=F32), buf(CHUNKS, GC, 128, dtype=F32),
        buf(8, 128, 128), buf(8, 128, dtype=F32), buf(8, 128, 128), buf(8, 8, 128, dtype=F32),
        buf(8, 128, 128, dtype=F32),
        buf(128, 128), buf(8, 128, dtype=F32), buf(NY, 128, 128), buf(NY, 8, 128, dtype=F32),
        buf(8, 128, 128), buf(8, 128, 128),
        buf(ROWS, GC), buf(4, ROWS, DB), buf(4, ROWS, DB), buf(4, ROWS, DB, dtype=F32),
        buf(ROWS, DB), buf(2, ROWS // 2, DB), buf(2, ROWS, DB), buf(2, ROWS, DB),
        dma((5,)), dma((5, 32)), dma((5, 32)), dma((13,)), dma((13,)), dma, dma,
        dma((2, NZ)), dma((2, NZ)), dma((2, NY)), dma((2, NY)), dma((NZ,)), dma((NZ,)),
        dma((4,)), dma((4,)), dma((6,)), dma((6,)),
    ]
    return pl.pallas_call(
        kernel,
        out_shape=jax.ShapeDtypeStruct((ROWS, DB), BF16),
        in_specs=[any_space] * 4 + [vmem] * 7,
        out_specs=vmem,
        scratch_shapes=scratch,
        compiler_params=pltpu.CompilerParams(
            collective_id=0, has_side_effects=True, vmem_limit_bytes=64 * 1024 * 1024 - 65536
        ),
    )(
        tokens, w_in.reshape(SUB, GC + CC), w_dt.T, w_out.reshape(GC, 4096),
        norm_gain.reshape(1, 4096), dt_bias.reshape(1, NH), a_log.reshape(1, NH), d_skip.reshape(1, NH),
        conv_w.reshape(4, CC), conv_b, gate_gain,
    )


def solution(mesh):
    in_specs = (
        P("seq", "head"), P(), P("seq", "head", None), P("seq", "head"), P("head"), P("head"), P("head"),
        P(None, "head", None), P("head", None), P("head", None), P("head", None, None),
    )
    return jax.shard_map(body, mesh=mesh, in_specs=in_specs, out_specs=P("seq", "head"), check_vma=False)
```

```python
import heapq
import itertools

import jax
import jax.numpy as jnp
from jax import lax
from jax.experimental import pallas as pl
from jax.experimental.pallas import tpu as pltpu
from jax.sharding import PartitionSpec as P

EPS = 1e-05
HIGHEST = lax.Precision.HIGHEST
MESH = pl.DeviceIdType.MESH
F32 = jnp.float32
BF16 = jnp.bfloat16

NY, NZ, NX = 4, 8, 4
ROWS = 384
HALF = ROWS // 2
DB = 512
SUB = 128
CC = 1280
GC = 1024
G1, G2 = 512, 512
NH = 16
CHUNKS = 3

STREAMS = (
    ("c", 0, 0, 64, True),
    ("c", 1, 0, 64, False),
    ("g1", 0, 0, 64, True),
    ("g1", 1, 0, 64, True),
    ("g2", 0, 0, 64, True),
    ("g2", 1, 0, 64, False),
)
WIDTH = {"c": CC, "g1": G1, "g2": G2}
FIRST = {"c": GC, "g1": 0, "g2": G1}


def children(stream, dy, dz):
    along_z, flip = STREAMS[stream][4], stream in (2, 3)
    out = []
    if along_z:
        up, down = (3, 4) if flip else (4, 3)
        if dy == 0:
            if 0 <= dz < up:
                out.append((0, dz + 1, "z+"))
            if 0 <= -dz < down:
                out.append((0, dz - 1, "z-"))
            out.append((1, dz, "y"))
    else:
        if (dy, dz) == (0, 0):
            out.append((1, 0, "y"))
        up, down = (4, 3) if (dy == 0) != flip else (3, 4)
        if 0 <= dz < up:
            out.append((dy, dz + 1, "z+"))
        if 0 <= -dz < down:
            out.append((dy, dz - 1, "z-"))
    return out


STARTS = {20: (2, 3), 44: (4, 5)}


def plan():
    free = dict.fromkeys(("y", "z+", "z-", "x+", "x-"), 0.0)
    events, done, order, tick = [], {}, [], itertools.count()
    left = {"c": 30, "g1": 30, "g2": 30, "tok": 12}
    taken = {"ring": 0}
    rate = 45000.0

    def later(t, item):
        heapq.heappush(events, (t, next(tick), item))

    def send(t, link, size, item):
        free[link] = max(t, free[link]) + size / rate
        later(free[link] + 2.2, item)

    def ring(t, stream, dy, dz):
        kind, _, _, rows, _ = STREAMS[stream]
        for a, b, d in children(stream, dy, dz):
            send(t, d, rows * WIDTH[kind] * 2, ("ring", stream, a, b))

    piece = HALF * DB * 2
    for item, t in ((("tin", 0), 10.0), (("tin", 1), 12.0), (("own", 0), 1.5), (("fold", 1), 9.5)):
        later(t, item)
    fold_at = {"g1": 20.0, "g2": 21.0}

    tiles = (4, 0, 1, 2, 3)
    units = [(("norm", i), 0.65, [("tok",)] if i == 0 else [("norm", i - 1)]) for i in range(4)]
    units += [(("prefix",), 0.4, [("ex1",)]), (("back",), 0.4, [("ex2",)])]
    units += [(("ends",), 0.2, [("state", i) for i in range(4)])]
    units += [(("dt",), 1.2, [("c",), ("norm", 3)]), (("mats",), 5.2, [("dt",)])]
    units += [(("state", i), 0.7, [("conv", i), ("conv", 4), ("prep",)]) for i in range(4)]
    units += [(("conv", i), 0.5, [("halo", i), ("chan", i)]) for i in tiles]
    units += [(("chan", i), 0.1, [("ch", i)]) for i in tiles]
    units += [(("prep",), 0.8, [("raw",)])]
    units += [(("carry",), 1.4, [("ex3",)] + [("inner", q, j) for q in range(CHUNKS) for j in range(4)])]
    units += [(("gate", i), 0.35, [("carry",), ("g", i)]) for i in range(4)]
    units += [(("gmats", 0), 1.9, [("g1",), ("mats",)]), (("gmats", 1), 1.9, [("g2",), ("mats",)])]
    units += [(("inner", q, j), 0.45, [("state", i) for i in range(4)]) for q in range(CHUNKS) for j in range(4)]

    now = 0.0
    while events or units:
        ready = [e for e in events if e[0] <= now]
        if ready:
            e = min(ready)
            events.remove(e)
            item = e[2]
            if item[0] == "ring":
                order.append(item)
                stream = item[1]
                kind = STREAMS[stream][0]
                left[kind] -= 1
                if not left[kind]:
                    later(now + (1.5 if kind == "c" else 3.0), ("flag", (kind,)))
                ring(now, *item[1:])
                taken["ring"] += 1
                for late in STARTS.get(taken["ring"], ()):
                    order.append(("begin", late))
                    ring(max(now, fold_at[STREAMS[late][0]]), late, 0, 0)
            elif item[0] in ("own", "fold"):
                order.append(("begin", item[1]))
                ring(now, item[1], 0, 0)
            elif item[0] == "tin":
                order.append(item)
                k = item[1]
                for p in (0, 1):
                    send(now, "x+", piece, ("tr", -1, k, p))
                for p in (1, 0):
                    send(now, "x-", piece, ("tr", 1, k, p))
            elif item[0] == "tr":
                order.append(item)
                _, dx, k, p = item
                if dx < 0 and p == 0:
                    send(now, "x+", piece, ("ta", k, p))
                if dx > 0 and p == 1:
                    send(now, "x-", piece, ("ta", k, p))
                left["tok"] -= 1
            elif item[0] == "ta":
                order.append(item)
                left["tok"] -= 1
            elif item[0] == "flag":
                done[item[1]] = now
            if item[0] in ("tr", "ta") and not left["tok"]:
                done[("tok",)] = now
            now += 0.05
            continue
        todo = [u for u in units if all(n in done for n in u[2])]
        if todo:
            unit = todo[0]
            units.remove(unit)
            name = unit[0]
            order.append(name)
            now += unit[1]
            done[name] = now
            if name[0] == "mats":
                for i, tile in enumerate(tiles):
                    later(now + max(i - 1, 0), ("flag", ("ch", tile)))
                    later(now + max(i - 1, 0) + 1.0, ("flag", ("halo", tile)))
            if name[0] == "dt":
                later(now + 2.5, ("flag", ("raw",)))
            if name[0] == "gmats":
                for i in (0, 1):
                    later(now + 4.5, ("flag", ("g", 2 * name[1] + i)))
            if name[0] in ("state", "back"):
                size = 74000 if name[0] == "state" else 295000
                for link in ("z+", "z-"):
                    free[link] = max(now, free[link]) + size / rate
                if name[0] == "back":
                    later(max(free["z+"], free["z-"]) + 3.0, ("flag", ("ex3",)))
            if name[0] == "ends":
                later(max(free["z+"], free["z-"], now) + 3.0, ("flag", ("ex1",)))
            if name[0] == "prefix":
                later(now + 4.0, ("flag", ("ex2",)))
            continue
        if not events:
            raise ValueError("stuck")
        now = min(events)[0]
    return order


PLAN = plan()


def number(dy, dz):
    return dy * NZ + dz % NZ


def softplus(v):
    return jnp.maximum(v, 0.0) + jnp.log1p(jnp.exp(-jnp.abs(v)))


def silu(v):
    return v / (1.0 + jnp.exp(-v))


def dot_nt(a, b):
    return lax.dot_general(a, b, (((1,), (1,)), ((), ())), preferred_element_type=F32)


def dot_tn(a, b):
    return lax.dot_general(a, b, (((0,), (0,)), ((), ())), preferred_element_type=F32)


def kernel(
    tok_in, w_in, w_dt, w_out, norm_gain, dt_bias, a_log, d_skip, conv_w, conv_b, gate_gain,
    out_ref,
    tok, xn, wc, wg1, wg2, wd, wo, ch, gs, raw,
    chf, halo_out, halo_in, cv, ybuf, tt, ct, fs, scores,
    e_out, d_out, e_in, d_in, pre, row_out, rowd_out, row_in, rowd_in, back_out, sin,
    no, sib_out, sib_in, part, far_out, far_in, near_out, near_in,
    load_sem, w_send, w_recv, f_send, f_recv, d_send, d_recv, t_send, t_recv, c_send, c_recv, h_send, h_recv,
    s_send, s_recv, r_send, r_recv, b_send, b_recv, o_send, o_recv, x_send, x_recv,
):
    s = lax.axis_index("seq")
    hd = lax.axis_index("head")
    y, z = lax.div(s, NZ), lax.rem(s, NZ)
    x, c = lax.div(hd, 2), lax.rem(hd, 2)
    kind_of_row = lax.div(y, 2)
    home = c == kind_of_row
    away = c != kind_of_row

    def at_yz(dy, dz):
        return lax.rem(y + dy + 2 * NY, NY) * NZ + lax.rem(z + dz + 2 * NZ, NZ)

    def head_of(dx, core):
        return lax.rem(x + dx + NX, NX) * 2 + core

    other = (NY - 1 - y) * NZ + z
    mate = (y + 1 - 2 * lax.rem(y, 2)) * NZ + z
    sibling = (s, x * 2 + (1 - c))
    plus, minus = (s, head_of(1, c)), (s, head_of(-1, c))
    lent = lax.select(home, 0, 1)
    halo_to = (lax.rem(lax.select(home, s, other) + 1, NY * NZ), x * 2 + lax.select(home, c, 1 - c))
    earlier = lax.rem(s + NY * NZ - 1, NY * NZ)
    earlier_row = lax.div(earlier, NZ)
    earlier_home = lax.div(earlier_row, 2) == c
    halo_from = (
        lax.select(earlier_home, earlier, (NY - 1 - earlier_row) * NZ + lax.rem(earlier, NZ)),
        x * 2 + lax.select(earlier_home, c, 1 - c),
    )
    target = {"y": (mate, hd), "z+": (at_yz(0, 1), hd), "z-": (at_yz(0, -1), hd)}
    z_peers = [(at_yz(0, k), hd) for k in range(1, NZ)]
    y_peers = [(at_yz(k, 0), hd) for k in range(1, NY)]
    swap = (other, x * 2 + (1 - c))
    sent, sent_if = [], []

    def remote(src, dst, send, recv, where):
        return pltpu.make_async_remote_copy(
            src_ref=src, dst_ref=dst, send_sem=send, recv_sem=recv, device_id=where, device_id_type=MESH
        )

    def push(src, dst, send, recv, where):
        copy = remote(src, dst, send, recv, where)
        copy.start()
        sent.append(copy)

    def push_if(condition, src, dst, send, recv, where):
        copy = remote(src, dst, send, recv, where)
        pl.when(condition)(copy.start)
        sent_if.append((condition, copy))

    def arrived(ref, recv):
        remote(ref, ref, recv, recv, sibling).wait_recv()

    def arrived_if(condition, ref, recv):
        pl.when(condition)(remote(ref, ref, recv, recv, sibling).wait_recv)

    held = {"c": wc, "g1": wg1, "g2": wg2}

    def cols_in(kind):
        return pl.ds(FIRST[kind], WIDTH[kind])

    def row_of(dy, dz, partner):
        row = y + dy * (1 - 2 * lax.rem(y, 2))
        row = NY - 1 - row if partner else row
        return (row * NZ + lax.rem(z - dz + NZ, NZ)) * SUB

    def block(stream, dy, dz, core):
        kind, partner, first, rows, _ = STREAMS[stream]
        base = row_of(dy, dz, partner) + 64 * core + first
        return held[kind].at[pl.ds(pl.multiple_of(base, 16), rows), :]

    def dt_block(dy, dz, partner):
        return wd.at[:, pl.ds(pl.multiple_of(row_of(dy, dz, partner), SUB), SUB)]

    own_rows = pl.ds(pl.multiple_of(row_of(0, 0, 0), SUB), SUB)
    kinds = ("c", "g1", "g2")
    loads = {k: pltpu.make_async_copy(w_in.at[:, cols_in(k)], held[k].at[own_rows, :], load_sem.at[i]) for i, k in enumerate(kinds)}
    loads["dt"] = pltpu.make_async_copy(w_dt, wd.at[:, own_rows], load_sem.at[3])
    own_cols = pl.ds(pl.multiple_of(c * DB, DB), DB)
    sib_cols = pl.ds(pl.multiple_of((1 - c) * DB, DB), DB)
    loads["tok"] = pltpu.make_async_copy(tok_in, tok.at[x, :, own_cols], load_sem.at[4])
    wo_load = pltpu.make_async_copy(w_out, wo, load_sem.at[5])

    @pl.when(home)
    def _():
        for key in ("c", "dt", "tok", "g1", "g2"):
            loads[key].start()

    wo_load.start()

    barrier = pltpu.get_barrier_semaphore()
    peers = z_peers + y_peers + [plus, minus, sibling, halo_to, halo_from, swap]
    for peer in peers:
        pl.semaphore_signal(barrier, inc=1, device_id=peer, device_id_type=MESH)
    pl.semaphore_wait(barrier, len(peers))

    half = [pl.ds(0, HALF), pl.ds(HALF, HALF)]
    here = [(other, x * 2), (other, x * 2 + 1)]

    def fold(kind, index):
        push_if(home, w_in.at[:, cols_in(kind)], held[kind].at[own_rows, :], f_send.at[0, index], f_recv.at[0, index], sibling)
        for core in (0, 1):
            rows = pl.ds(64 * core, 64)
            there = pl.ds(pl.multiple_of(row_of(0, 0, 0) + 64 * core, 16), 64)
            push_if(
                away, w_in.at[rows, cols_in(kind)], held[kind].at[there, :],
                f_send.at[1 + core, index], f_recv.at[1, index], here[core],
            )

    def fold_dt():
        push_if(home, w_dt, wd.at[:, own_rows], f_send.at[0, 3], f_recv.at[0, 3], sibling)
        for core in (0, 1):
            push_if(away, w_dt, wd.at[:, own_rows], f_send.at[1 + core, 3], f_recv.at[1, 3], here[core])

    fold("c", 0)
    fold_dt()
    for k in (0, 1):
        rows = half[k]
        into = tok.at[x, rows, own_cols]
        push_if(away, tok_in.at[rows, :], into, t_send.at[14 + k], t_recv.at[14 + k], sibling)
        push_if(home, tok_in.at[rows, :], into, t_send.at[12 + k], t_recv.at[12 + k], (other, hd))
        push_if(away, tok_in.at[rows, :], into, t_send.at[12 + k], t_recv.at[14 + k], swap)
    fold("g1", 1)
    fold("g2", 2)

    def own_ready(kind, index):
        @pl.when(home)
        def _():
            loads[kind].wait()

        ref = wd.at[:, own_rows] if kind == "dt" else held[kind].at[own_rows, :]
        arrived_if(away, ref, f_recv.at[0, index])

    def partner_ready(kind, index):
        base = row_of(0, 0, 1)
        if kind == "dt":
            arrived(dt_block(0, 0, 1), f_recv.at[1, index])
        else:
            arrived(held[kind].at[pl.ds(pl.multiple_of(base + 64 * c, 16), 64), :], f_recv.at[1, index])

    def spread(stream, dy, dz):
        piece = block(stream, dy, dz, c)
        for a, b, d in children(stream, dy, dz):
            k = number(a, b)
            push(piece, piece, w_send.at[stream, k], w_recv.at[stream, k], target[d])
            if stream < 2:
                small = dt_block(dy, dz, stream)
                push(small, small, w_send.at[6 + stream, k], w_recv.at[6 + stream, k], target[d])
        if (dy, dz) != (0, 0) or STREAMS[stream][1]:
            k = number(dy, dz)
            push(piece, piece, d_send.at[stream, k], d_recv.at[stream, k], sibling)

    def all_here(streams):
        for stream in streams:
            for dy in (0, 1):
                for dz in range(NZ):
                    if (dy, dz) != (0, 0) or STREAMS[stream][1]:
                        arrived(block(stream, dy, dz, 1 - c), d_recv.at[stream, number(dy, dz)])

    def begin(stream):
        kind, partner = STREAMS[stream][:2]
        index = kinds.index(kind)
        if partner:
            partner_ready(kind, index)
            if stream == 1:
                partner_ready("dt", 3)
        else:
            own_ready(kind, index)
            if stream == 0:
                own_ready("dt", 3)
        spread(stream, 0, 0)

    def ring(stream, dy, dz):
        k = number(dy, dz)
        arrived(block(stream, dy, dz, c), w_recv.at[stream, k])
        if stream < 2:
            arrived(dt_block(dy, dz, stream), w_recv.at[6 + stream, k])
        spread(stream, dy, dz)

    def tok_piece(dx, k, p):
        return tok.at[lax.rem(x + dx + NX, NX), half[k], own_cols if p == 0 else sib_cols]

    def tok_in_here(k):
        if k == 0:

            @pl.when(home)
            def _():
                loads["tok"].wait()

        arrived_if(away, tok_piece(0, k, 0), t_recv.at[12 + k])
        arrived(tok_piece(0, k, 1), t_recv.at[14 + k])
        for p in (0, 1):
            piece = tok_piece(0, k, p)
            push(piece, piece, t_send.at[k * 2 + p], t_recv.at[k * 2 + p], plus)
        for p in (1, 0):
            piece = tok_piece(0, k, p)
            push(piece, piece, t_send.at[4 + k * 2 + p], t_recv.at[4 + k * 2 + p], minus)

    def tok_relay(dx, k, p):
        piece = tok_piece(dx, k, p)
        index = (0 if dx < 0 else 4) + k * 2 + p
        arrived(piece, t_recv.at[index])
        if dx < 0 and p == 0:
            push(piece, piece, t_send.at[8 + k], t_recv.at[8 + k], plus)
        if dx > 0 and p == 1:
            push(piece, piece, t_send.at[10 + k], t_recv.at[10 + k], minus)

    def tok_far(k, p):
        arrived(tok_piece(2, k, p), t_recv.at[(8 if p == 0 else 10) + k])

    def norm_rows(i, carry):
        rows = pl.ds(pl.multiple_of(i * 32, 32), 32)
        total = jnp.zeros((32, 1), F32)
        for h in range(8):
            v = tok[h // 2, rows, (h % 2) * DB : (h % 2 + 1) * DB].astype(F32)
            total = total + jnp.sum(v * v, axis=1, keepdims=True)
        scale = lax.rsqrt(total / (8 * DB) + EPS)
        for h in range(8):
            cols = slice((h % 2) * DB, (h % 2 + 1) * DB)
            v = tok[h // 2, rows, cols].astype(F32)
            xn[rows, h * DB : (h + 1) * DB] = (v * scale * norm_gain[:, h * DB : (h + 1) * DB]).astype(BF16)
        return carry

    def norm(i):
        lax.fori_loop(i * 3, i * 3 + 3, norm_rows, 0)

    def project(weights, first, width):
        cols = pl.ds(first, width)
        return jnp.dot(xn[...], weights[:, cols], preferred_element_type=F32).astype(BF16)

    def ship(buffer, tile, index):
        push_if(away, buffer.at[1, tile], buffer.at[0, tile], c_send.at[index], c_recv.at[index], swap)

    pending = []

    def channel_copies(tile):
        return (
            remote(halo_out.at[tile], halo_in.at[tile], h_send.at[tile], h_recv.at[tile], halo_to),
            remote(ch.at[1, tile], ch.at[0, tile], c_send.at[tile], c_recv.at[tile], swap),
        )

    def send_channels(tile):
        halo, rest = channel_copies(tile)
        halo.start()
        pl.when(away)(rest.start)

    def mats():
        all_here((0, 1))

        def one(i, carry):
            tile = lax.rem(i + 4, 5)

            @pl.when(i > 0)
            def _():
                send_channels(lax.rem(i + 3, 5))

            value = project(wc, pl.multiple_of(tile * 256, 256), 256)
            ch[lent, tile] = value
            halo_out[tile] = value[ROWS - 16 :, :]
            return carry

        lax.fori_loop(0, 5, one, 0)
        for tile in range(5):
            halo, rest = channel_copies(tile)
            sent.append(halo)
            sent_if.append((away, rest))
        pending.append(lambda: send_channels(3))

    def dt():
        raw[lent, 0] = dot_nt(wd[...], xn[...])
        pending.append(lambda: ship(raw, 0, 5))

    def gate_copy(tile):
        return remote(gs.at[1, tile], gs.at[0, tile], c_send.at[6 + tile], c_recv.at[6 + tile], swap)

    def gmats(second):
        all_here((4, 5) if second else (2, 3))
        base = 2 * second
        value = project(wg2 if second else wg1, 0, 512)
        for tile in (0, 1):
            gs[lent, base + tile] = value[:, tile * 256 : (tile + 1) * 256]
            sent_if.append((away, gate_copy(base + tile)))

        @pl.when(away)
        def _():
            gate_copy(base).start()
            gate_copy(base + 1).start()

    def chan(tile):
        arrived_if(away, ch.at[0, tile], c_recv.at[tile])
        chf[8:, tile * 256 : (tile + 1) * 256] = ch[0, tile].astype(F32)

    def column_of(ref):
        wide = jnp.concatenate([ref[...], jnp.zeros((1, 128 - NH), F32)], axis=1)
        return jnp.transpose(jnp.broadcast_to(wide, (128, 128)))[:NH, :1]

    row_id = lax.broadcasted_iota(jnp.int32, (128, 128), 0)
    lane_id = lax.broadcasted_iota(jnp.int32, (128, 128), 1)
    first_half = lane_id < 64
    upper_rows = row_id < 64

    def prep():
        arrived_if(away, raw.at[0, 0], c_recv.at[5])
        step = softplus(raw[0, 0] + column_of(dt_bias))
        decay = -jnp.exp(column_of(a_log)) * step
        upper = jnp.where(row_id <= lane_id, 1.0, 0.0).astype(F32)
        for q in range(CHUNKS):
            span = slice(q * 128, (q + 1) * 128)
            cum = jnp.dot(decay[:, span], upper, precision=HIGHEST, preferred_element_type=F32)
            to_end = jnp.exp(cum[:, 127:128] - cum) * step[:, span]
            ct[q] = cum
            stacked = jnp.concatenate(
                [cum, to_end, step[:, span], jnp.exp(cum), jnp.zeros((64, 128), F32)], axis=0
            )
            tt[q] = jnp.transpose(stacked)
        d_out[...] = jnp.broadcast_to(tt[0, 127:128, :] + tt[1, 127:128, :] + tt[2, 127:128, :], (8, 128))
        d_in[z] = d_out[...]

    def conv(tile):
        arrived(halo_in.at[tile], h_recv.at[tile])
        wide = slice(tile * 256, (tile + 1) * 256)
        chf[:8, wide] = jnp.where(s > 0, halo_in[tile, 8:16, :].astype(F32), 0.0)
        for cols in (slice(tile * 256, tile * 256 + 128), slice(tile * 256 + 128, tile * 256 + 256)):
            for q in range(CHUNKS):
                total = conv_b[:, cols] + jnp.zeros((128, 128), F32)
                for k in range(4):
                    total = total + conv_w[k, :, cols] * chf[q * 128 + 5 + k : q * 128 + 133 + k, cols]
                cv[q * 128 : (q + 1) * 128, cols] = silu(total).astype(BF16)

    def pair_cols(table, base, j):
        return jnp.where(
            first_half, table[:, base + 2 * j : base + 2 * j + 1], table[:, base + 2 * j + 1 : base + 2 * j + 2]
        )

    def pair_rows(row, j):
        return jnp.where(upper_rows, jnp.exp(row[:, 2 * j : 2 * j + 1]), jnp.exp(row[:, 2 * j + 1 : 2 * j + 2]))

    def end_states(tile):
        for j in (2 * tile, 2 * tile + 1):
            cols = slice(j * 128, (j + 1) * 128)
            for q in range(CHUNKS):
                span = slice(q * 128, (q + 1) * 128)
                weighted = (cv[span, cols].astype(F32) * pair_cols(tt[q], 16, j)).astype(BF16)
                fs[q, cols, :] = dot_tn(weighted, cv[span, 1024:1152])
            total = fs[1, cols, :] + pair_rows(tt[1, 127:128, :], j) * fs[0, cols, :]
            e_out[j] = (fs[2, cols, :] + pair_rows(tt[2, 127:128, :], j) * total).astype(BF16)

        def go():
            for j in (2 * tile, 2 * tile + 1):
                peer = (y * NZ + j, hd)
                push_if(z != j, e_out.at[j], e_in.at[z], s_send.at[0, j], s_recv.at[0, z], peer)
                push_if(z != j, d_out, d_in.at[z], s_send.at[1, j], s_recv.at[1, z], peer)

        pending.append(go)

    def inner(q, part_of):
        span = slice(q * 128, (q + 1) * 128)
        if part_of == 0:
            scores[...] = jnp.where(row_id >= lane_id, dot_nt(cv[span, 1152:1280], cv[span, 1024:1152]), 0.0)
        table = tt[q]
        for j in (2 * part_of, 2 * part_of + 1):
            cols = slice(j * 128, (j + 1) * 128)
            v = cv[span, cols].astype(F32)
            stepped = v * pair_cols(table, 32, j)
            values = jnp.concatenate(
                [jnp.where(first_half, stepped, 0.0), jnp.where(first_half, 0.0, stepped)], axis=0
            ).astype(BF16)
            weights = []
            for h in (2 * j, 2 * j + 1):
                gap = jnp.minimum(table[:, h : h + 1] - ct[q, h : h + 1, :], 0.0)
                weights.append((scores[...] * jnp.exp(gap)).astype(BF16))
            within = jnp.dot(jnp.concatenate(weights, axis=1), values, preferred_element_type=F32)
            skip = jnp.where(first_half[:1], d_skip[:, 2 * j : 2 * j + 1], d_skip[:, 2 * j + 1 : 2 * j + 2])
            ybuf[span, cols] = within + skip * v

    def ends():
        e_in[z] = e_out[z]

    lane_row = lax.broadcasted_iota(jnp.int32, (1, 128), 1)

    def pick(row, lane):
        return jnp.sum(jnp.where(lane_row == lane, row, 0.0), axis=1, keepdims=True)

    def factor(pair):
        return jnp.where(upper_rows[:, :1], jnp.exp(pair[0]), jnp.exp(pair[1]))

    before = []

    def prefix():
        for k in range(1, NZ):
            source = lax.rem(z + NZ - k, NZ)
            arrived(e_in.at[source], s_recv.at[0, source])
            arrived(d_in.at[source], s_recv.at[1, source])
        running = jnp.zeros((128, 128), F32)
        gone = (jnp.zeros((1, 1), F32), jnp.zeros((1, 1), F32))
        for k in range(NZ):
            pre[k] = running
            before.append(gone)
            row = d_in[k, :1, :]
            pair = (pick(row, 2 * z), pick(row, 2 * z + 1))
            running = factor(pair) * running + e_in[k].astype(F32)
            gone = (gone[0] + pair[0], gone[1] + pair[1])
        row_out[...] = running.astype(BF16)
        rowd_out[...] = jnp.broadcast_to(jnp.where(lane_row == 0, gone[0], gone[1]), (8, 128))
        row_in[y] = running.astype(BF16)
        rowd_in[y] = jnp.broadcast_to(jnp.where(lane_row == 0, gone[0], gone[1]), (8, 128))

        def go():
            for k in range(1, NY):
                push(row_out, row_in.at[y], r_send.at[0, k], r_recv.at[0, k], y_peers[k - 1])
                push(rowd_out, rowd_in.at[y], r_send.at[1, k], r_recv.at[1, k], y_peers[k - 1])

        pending.append(go)

    def back():
        for k in range(1, NY):
            source = lax.rem(y + NY - k, NY)
            arrived(row_in.at[source], r_recv.at[0, k])
            arrived(rowd_in.at[source], r_recv.at[1, k])
        entering = jnp.zeros((128, 128), F32)
        for k in range(NY):
            row = rowd_in[k, :1, :]
            moved = factor((row[:, 0:1], row[:, 1:2])) * entering + row_in[k].astype(F32)
            entering = jnp.where(k < y, moved, entering)
        for k in range(NZ):
            back_out[k] = (factor(before[k]) * entering + pre[k]).astype(BF16)
        sin[z] = back_out[z]

        def go():
            for k in range(1, NZ):
                peer = lax.rem(z + k, NZ)
                push(back_out.at[peer], sin.at[z], b_send.at[k], b_recv.at[k], z_peers[k - 1])

        pending.append(go)

    def carry():
        for k in range(1, NZ):
            arrived(sin.at[lax.rem(z + NZ - k, NZ)], b_recv.at[k])
        for j in range(8):
            cols = slice(j * 128, (j + 1) * 128)
            entering = sin[j].astype(F32)
            for q in range(CHUNKS):
                span = slice(q * 128, (q + 1) * 128)
                across = dot_nt(cv[span, 1152:1280], entering.astype(BF16))
                ybuf[span, cols] += pair_cols(tt[q], 48, j) * across
                if q < CHUNKS - 1:
                    entering = pair_rows(tt[q, 127:128, :], j) * entering + fs[q, cols, :]

    squares = [jnp.zeros((ROWS, 1), F32)]

    def gate(tile):
        cols = slice(tile * 256, (tile + 1) * 256)
        arrived_if(away, gs.at[0, tile], c_recv.at[6 + tile])
        gated = ybuf[:, cols] * silu(gs[0, tile].astype(F32))
        ybuf[:, cols] = gated
        squares[0] = squares[0] + jnp.sum(gated * gated, axis=1, keepdims=True)

    steps = {
        "begin": begin, "ring": ring, "tin": tok_in_here, "tr": tok_relay, "ta": tok_far, "norm": norm, "mats": mats,
        "dt": dt, "gmats": gmats, "chan": chan, "prep": prep, "conv": conv, "state": end_states, "inner": inner,
        "ends": ends, "prefix": prefix, "back": back, "carry": carry, "gate": gate,
    }
    for step in PLAN:
        later, pending[:] = list(pending), []
        for go in later:
            go()
        steps[step[0]](*step[1:])
    for go in pending:
        go()
    scale = lax.rsqrt(squares[0] / GC + EPS)

    def norm_tile(i, carry):
        cols = pl.ds(pl.multiple_of(i * 128, 128), 128)
        no[:, cols] = (ybuf[:, cols] * scale * gate_gain[:, cols]).astype(BF16)
        return carry

    lax.fori_loop(0, 8, norm_tile, 0)
    wo_load.wait()

    def term(dx, core, into):
        cols = pl.ds(pl.multiple_of(head_of(dx, core) * DB, DB), DB)
        into[...] = jnp.dot(no[...], wo[:, cols], preferred_element_type=F32).astype(into.dtype)

    top, low = half

    def to_sibling(r):
        term(r, 1 - c, sib_out.at[r])

    def keep(r):
        term(r, c, part.at[r])

    def send_sibling(r):
        push(sib_out.at[r], sib_in.at[r], o_send.at[r], o_recv.at[r], sibling)

    def chip_sum(r, rows):
        return part[r, rows, :] + sib_in[r, rows, :].astype(F32)

    to_sibling(2)
    keep(2)
    send_sibling(2)
    to_sibling(1)
    to_sibling(3)
    send_sibling(1)
    keep(1)
    send_sibling(3)
    arrived(sib_in.at[2], o_recv.at[2])
    far_out[...] = chip_sum(2, slice(None)).astype(BF16)
    keep(3)
    push(far_out.at[top, :], far_in.at[0], x_send.at[0], x_recv.at[0], plus)
    push(far_out.at[low, :], far_in.at[1], x_send.at[1], x_recv.at[1], minus)
    arrived(sib_in.at[1], o_recv.at[1])
    near_out[0, low, :] = chip_sum(1, low).astype(BF16)
    arrived(sib_in.at[3], o_recv.at[3])
    near_out[1, top, :] = chip_sum(3, top).astype(BF16)
    push(near_out.at[0, low, :], near_in.at[0, low, :], x_send.at[2], x_recv.at[2], plus)
    to_sibling(0)
    push(near_out.at[1, top, :], near_in.at[1, top, :], x_send.at[3], x_recv.at[3], minus)
    keep(0)
    send_sibling(0)
    arrived(far_in.at[0], x_recv.at[0])
    near_out[0, top, :] = (chip_sum(1, top) + far_in[0].astype(F32)).astype(BF16)
    push(near_out.at[0, top, :], near_in.at[0, top, :], x_send.at[4], x_recv.at[4], plus)
    arrived(far_in.at[1], x_recv.at[1])
    near_out[1, low, :] = (chip_sum(3, low) + far_in[1].astype(F32)).astype(BF16)
    push(near_out.at[1, low, :], near_in.at[1, low, :], x_send.at[5], x_recv.at[5], minus)
    arrived(sib_in.at[0], o_recv.at[0])
    part[0] = chip_sum(0, slice(None))
    arrived(near_in.at[0, low, :], x_recv.at[2])
    arrived(near_in.at[1, top, :], x_recv.at[3])
    arrived(near_in.at[0, top, :], x_recv.at[4])
    arrived(near_in.at[1, low, :], x_recv.at[5])
    out_ref[...] = (part[0] + near_in[0].astype(F32) + near_in[1].astype(F32)).astype(BF16)
    for copy in sent:
        copy.wait_send()
    for condition, copy in sent_if:
        pl.when(condition)(copy.wait_send)


def body(tokens, norm_gain, w_in, w_dt, dt_bias, a_log, d_skip, conv_w, conv_b, gate_gain, w_out):
    any_space = pl.BlockSpec(memory_space=pl.ANY)
    vmem = pl.BlockSpec(memory_space=pltpu.VMEM)
    dma = pltpu.SemaphoreType.DMA

    def buf(*shape, dtype=BF16):
        return pltpu.VMEM(shape, dtype)

    scratch = [
        buf(NX, ROWS, 2 * DB), buf(ROWS, 4096), buf(4096, CC), buf(4096, G1), buf(4096, G2),
        buf(NH, 4096), buf(GC, 4096), buf(2, 5, ROWS, 256), buf(2, 4, ROWS, 256),
        buf(2, 1, NH, ROWS, dtype=F32),
        buf(ROWS + 8, CC, dtype=F32), buf(5, 16, 256), buf(5, 16, 256), buf(ROWS, CC), buf(ROWS, GC, dtype=F32),
        buf(CHUNKS, 128, 128, dtype=F32), buf(CHUNKS, NH, 128, dtype=F32), buf(CHUNKS, GC, 128, dtype=F32), buf(128, 128, dtype=F32),
        buf(8, 128, 128), buf(8, 128, dtype=F32), buf(8, 128, 128), buf(8, 8, 128, dtype=F32),
        buf(8, 128, 128, dtype=F32),
        buf(128, 128), buf(8, 128, dtype=F32), buf(NY, 128, 128), buf(NY, 8, 128, dtype=F32),
        buf(8, 128, 128), buf(8, 128, 128),
        buf(ROWS, GC), buf(4, ROWS, DB), buf(4, ROWS, DB), buf(4, ROWS, DB, dtype=F32),
        buf(ROWS, DB), buf(2, ROWS // 2, DB), buf(2, ROWS, DB), buf(2, ROWS, DB),
        dma((6,)), dma((8, 16)), dma((8, 16)), dma((3, 4)), dma((2, 4)), dma((6, 16)), dma((6, 16)),
        dma((16,)), dma((16,)), dma((10,)), dma((10,)), dma((5,)), dma((5,)),
        dma((2, NZ)), dma((2, NZ)), dma((2, NY)), dma((2, NY)), dma((NZ,)), dma((NZ,)),
        dma((4,)), dma((4,)), dma((6,)), dma((6,)),
    ]
    return pl.pallas_call(
        kernel,
        out_shape=jax.ShapeDtypeStruct((ROWS, DB), BF16),
        in_specs=[any_space] * 4 + [vmem] * 7,
        out_specs=vmem,
        scratch_shapes=scratch,
        compiler_params=pltpu.CompilerParams(
            collective_id=0, has_side_effects=True, vmem_limit_bytes=64 * 1024 * 1024 - 65536
        ),
    )(
        tokens, w_in.reshape(SUB, GC + CC), w_dt.T, w_out.reshape(GC, 4096),
        norm_gain.reshape(1, 4096), dt_bias.reshape(1, NH), a_log.reshape(1, NH), d_skip.reshape(1, NH),
        conv_w, conv_b, gate_gain,
    )


def solution(mesh):
    in_specs = (
        P("seq", "head"), P(), P("seq", "head", None), P("seq", "head"), P("head"), P("head"), P("head"),
        P(None, "head", None), P("head", None), P("head", None), P("head", None, None),
    )
    return jax.shard_map(body, mesh=mesh, in_specs=in_specs, out_specs=P("seq", "head"), check_vma=False)
```

```python
import heapq
import itertools

import jax
import jax.numpy as jnp
from jax import lax
from jax.experimental import pallas as pl
from jax.experimental.pallas import tpu as pltpu
from jax.sharding import PartitionSpec as P

EPS = 1e-05
HIGHEST = lax.Precision.HIGHEST
MESH = pl.DeviceIdType.MESH
F32 = jnp.float32
BF16 = jnp.bfloat16

NY, NZ, NX = 4, 8, 4
ROWS = 384
HALF = ROWS // 2
DB = 512
SUB = 128
CC = 1280
GC = 1024
G1, G2 = 512, 512
NH = 16
CHUNKS = 3

STREAMS = (
    ("c", 0, 0, 64, True),
    ("c", 1, 0, 64, False),
    ("g1", 0, 0, 64, True),
    ("g1", 1, 0, 64, True),
    ("g2", 0, 0, 64, True),
    ("g2", 1, 0, 64, False),
)
WIDTH = {"c": CC, "g1": G1, "g2": G2}
FIRST = {"c": GC, "g1": 0, "g2": G1}


def children(stream, dy, dz):
    along_z, flip = STREAMS[stream][4], stream in (2, 3)
    out = []
    if along_z:
        up, down = (3, 4) if flip else (4, 3)
        if dy == 0:
            if 0 <= dz < up:
                out.append((0, dz + 1, "z+"))
            if 0 <= -dz < down:
                out.append((0, dz - 1, "z-"))
            out.append((1, dz, "y"))
    else:
        if (dy, dz) == (0, 0):
            out.append((1, 0, "y"))
        up, down = (4, 3) if (dy == 0) != flip else (3, 4)
        if 0 <= dz < up:
            out.append((dy, dz + 1, "z+"))
        if 0 <= -dz < down:
            out.append((dy, dz - 1, "z-"))
    return out


STARTS = {26: (2, 3), 32: (4, 5)}
EX, HAND = (1.0, 3.5, 1.0), {"c": 1.5, "g1": 3.0, "g2": 3.0}
TIN, FOLD, XRATE = (12.0, 14.0), 10.0, (80000.0, 45000.0)


def plan():
    free = dict.fromkeys(("y", "z+", "z-", "x+", "x-"), 0.0)
    events, done, order, tick = [], {}, [], itertools.count()
    left = {"c": 30, "g1": 30, "g2": 30, "tok": 12}
    taken = {"ring": 0}
    rate = 45000.0

    def later(t, item):
        heapq.heappush(events, (t, next(tick), item))

    def send(t, link, size, item, speed=45000.0):
        free[link] = max(t, free[link]) + size / speed
        later(free[link] + 2.2, item)

    def ring(t, stream, dy, dz):
        kind, _, _, rows, _ = STREAMS[stream]
        for a, b, d in children(stream, dy, dz):
            send(t, d, rows * WIDTH[kind] * 2, ("ring", stream, a, b))

    piece = HALF * DB * 2
    for item, t in ((("tinh", 0), 3.0), (("tinh", 1), 3.5), (("tin", 0), TIN[0]), (("tin", 1), TIN[1]), (("own", 0), 1.5), (("fold", 1), FOLD)):
        later(t, item)
    fold_at = {"g1": 20.0, "g2": 21.0}

    tiles = (4, 0, 1, 2, 3)
    units = [(("norm", i), 0.65, [("tok",)] if i == 0 else [("norm", i - 1)]) for i in range(4)]
    units += [(("prefix",), 0.4, [("ex1",)]), (("back",), 0.4, [("ex2",)])]
    units += [(("ends",), 0.2, [("state", i) for i in range(4)])]
    units += [(("dt",), 1.2, [("c",), ("norm", 3)]), (("mats", 0), 3.6, [("dt",)]), (("mats", 1), 1.9, [("mats", 0)])]
    units += [(("state", i), 0.7, [("conv", i), ("conv", 4), ("prep",)]) for i in range(4)]
    units += [(("conv", i), 0.5, [("halo", i), ("chan", i)]) for i in tiles]
    units += [(("chan", i), 0.1, [("ch", i)]) for i in tiles]
    units += [(("prep",), 0.8, [("raw",)])]
    units += [(("carry",), 1.4, [("ex3",)] + [("inner", q, j) for q in range(CHUNKS) for j in range(4)])]
    units += [(("gate", i), 0.35, [("carry",), ("g", i)]) for i in range(4)]
    units += [(("gmats", 0), 1.9, [("g1",), ("mats", 1)]), (("gmats", 1), 1.9, [("g2",), ("mats", 1)])]
    units += [(("inner", q, j), 0.45, [("state", i) for i in range(4)]) for q in range(CHUNKS) for j in range(4)]

    now = 0.0
    while events or units:
        ready = [e for e in events if e[0] <= now]
        if ready:
            e = min(ready)
            events.remove(e)
            item = e[2]
            if item[0] == "ring":
                order.append(item)
                stream = item[1]
                kind = STREAMS[stream][0]
                left[kind] -= 1
                if not left[kind]:
                    later(now + HAND[kind], ("flag", (kind,)))
                ring(now, *item[1:])
                taken["ring"] += 1
                for late in STARTS.get(taken["ring"], ()):
                    order.append(("begin", late))
                    ring(max(now, fold_at[STREAMS[late][0]]), late, 0, 0)
            elif item[0] in ("own", "fold"):
                order.append(("begin", item[1]))
                ring(now, item[1], 0, 0)
            elif item[0] == "tinh":
                order.append(item)
            elif item[0] == "tin":
                order.append(item)
                k = item[1]
                for p in (0, 1):
                    send(now, "x+", piece, ("tr", -1, k, p), XRATE[0])
                for p in (1, 0):
                    send(now, "x-", piece, ("tr", 1, k, p), XRATE[0])
            elif item[0] == "tr":
                order.append(item)
                _, dx, k, p = item
                if dx < 0 and p == 0:
                    send(now, "x+", piece, ("ta", k, p), XRATE[1])
                if dx > 0 and p == 1:
                    send(now, "x-", piece, ("ta", k, p), XRATE[1])
                left["tok"] -= 1
            elif item[0] == "ta":
                order.append(item)
                left["tok"] -= 1
            elif item[0] == "flag":
                done[item[1]] = now
            if item[0] in ("tr", "ta") and not left["tok"]:
                done[("tok",)] = now
            now += 0.05
            continue
        todo = [u for u in units if all(n in done for n in u[2])]
        if todo:
            unit = todo[0]
            units.remove(unit)
            name = unit[0]
            order.append(name)
            now += unit[1]
            done[name] = now
            if name[0] == "mats":
                for i, tile in enumerate((2, 3) if name[1] else (4, 0, 1)):
                    wait = 3.0 + 1.8 * i if name[1] else 2.0 + i
                    later(now + wait, ("flag", ("ch", tile)))
                    later(now + wait + 0.5, ("flag", ("halo", tile)))
            if name[0] == "dt":
                later(now + 2.5, ("flag", ("raw",)))
            if name[0] == "gmats":
                for i in (0, 1):
                    later(now + 4.5, ("flag", ("g", 2 * name[1] + i)))
            if name[0] in ("state", "back"):
                size = 74000 if name[0] == "state" else 295000
                for link in ("z+", "z-"):
                    free[link] = max(now, free[link]) + size / rate
                if name[0] == "back":
                    later(max(free["z+"], free["z-"]) + EX[2], ("flag", ("ex3",)))
            if name[0] == "ends":
                later(max(free["z+"], free["z-"], now) + EX[0], ("flag", ("ex1",)))
            if name[0] == "prefix":
                later(now + EX[1], ("flag", ("ex2",)))
            continue
        if not events:
            raise ValueError("stuck")
        now = min(events)[0]
    return order


PLAN = plan()


def number(dy, dz):
    return dy * NZ + dz % NZ


def softplus(v):
    return jnp.maximum(v, 0.0) + jnp.log1p(jnp.exp(-jnp.abs(v)))


def silu(v):
    return v / (1.0 + jnp.exp(-v))


def dot_nt(a, b):
    return lax.dot_general(a, b, (((1,), (1,)), ((), ())), preferred_element_type=F32)


def dot_tn(a, b):
    return lax.dot_general(a, b, (((0,), (0,)), ((), ())), preferred_element_type=F32)


def kernel(
    tok_in, w_in, w_dt, w_out, norm_gain, dt_bias, a_log, d_skip, conv_w, conv_b, gate_gain,
    out_ref,
    tok, xn, wc, wg1, wg2, wd, wo, ch, gs, raw,
    chf, halo_out, halo_in, cv, ybuf, tt, ct, fs, scores,
    e_out, d_out, e_in, d_in, pre, row_out, rowd_out, row_in, rowd_in, back_out, sin,
    no, sib_out, sib_in, part, far_out, far_in, near_out, near_in,
    load_sem, w_send, w_recv, f_send, f_recv, d_send, d_recv, t_send, t_recv, c_send, c_recv, h_send, h_recv,
    s_send, s_recv, r_send, r_recv, b_send, b_recv, o_send, o_recv, x_send, x_recv,
):
    s = lax.axis_index("seq")
    hd = lax.axis_index("head")
    y, z = lax.div(s, NZ), lax.rem(s, NZ)
    x, c = lax.div(hd, 2), lax.rem(hd, 2)
    kind_of_row = lax.div(y, 2)
    home = c == kind_of_row
    away = c != kind_of_row

    def at_yz(dy, dz):
        return lax.rem(y + dy + 2 * NY, NY) * NZ + lax.rem(z + dz + 2 * NZ, NZ)

    def head_of(dx, core):
        return lax.rem(x + dx + NX, NX) * 2 + core

    other = (NY - 1 - y) * NZ + z
    mate = (y + 1 - 2 * lax.rem(y, 2)) * NZ + z
    sibling = (s, x * 2 + (1 - c))
    plus, minus = (s, head_of(1, c)), (s, head_of(-1, c))
    lent = lax.select(home, 0, 1)
    halo_to = (lax.rem(lax.select(home, s, other) + 1, NY * NZ), x * 2 + lax.select(home, c, 1 - c))
    earlier = lax.rem(s + NY * NZ - 1, NY * NZ)
    earlier_row = lax.div(earlier, NZ)
    earlier_home = lax.div(earlier_row, 2) == c
    halo_from = (
        lax.select(earlier_home, earlier, (NY - 1 - earlier_row) * NZ + lax.rem(earlier, NZ)),
        x * 2 + lax.select(earlier_home, c, 1 - c),
    )
    target = {"y": (mate, hd), "z+": (at_yz(0, 1), hd), "z-": (at_yz(0, -1), hd)}
    z_peers = [(at_yz(0, k), hd) for k in range(1, NZ)]
    y_peers = [(at_yz(k, 0), hd) for k in range(1, NY)]
    swap = (other, x * 2 + (1 - c))
    sent, sent_if = [], []

    def remote(src, dst, send, recv, where):
        return pltpu.make_async_remote_copy(
            src_ref=src, dst_ref=dst, send_sem=send, recv_sem=recv, device_id=where, device_id_type=MESH
        )

    def push(src, dst, send, recv, where):
        copy = remote(src, dst, send, recv, where)
        copy.start()
        sent.append(copy)

    def push_if(condition, src, dst, send, recv, where):
        copy = remote(src, dst, send, recv, where)
        pl.when(condition)(copy.start)
        sent_if.append((condition, copy))

    def arrived(ref, recv):
        remote(ref, ref, recv, recv, sibling).wait_recv()

    def arrived_if(condition, ref, recv):
        pl.when(condition)(remote(ref, ref, recv, recv, sibling).wait_recv)

    held = {"c": wc, "g1": wg1, "g2": wg2}

    def cols_in(kind):
        return pl.ds(FIRST[kind], WIDTH[kind])

    def row_of(dy, dz, partner):
        row = y + dy * (1 - 2 * lax.rem(y, 2))
        row = NY - 1 - row if partner else row
        return (row * NZ + lax.rem(z - dz + NZ, NZ)) * SUB

    def block(stream, dy, dz, core):
        kind, partner, first, rows, _ = STREAMS[stream]
        base = row_of(dy, dz, partner) + 64 * core + first
        return held[kind].at[pl.ds(pl.multiple_of(base, 16), rows), :]

    def dt_block(dy, dz, partner):
        return wd.at[:, pl.ds(pl.multiple_of(row_of(dy, dz, partner), SUB), SUB)]

    own_rows = pl.ds(pl.multiple_of(row_of(0, 0, 0), SUB), SUB)
    kinds = ("c", "g1", "g2")
    loads = {k: pltpu.make_async_copy(w_in.at[:, cols_in(k)], held[k].at[own_rows, :], load_sem.at[i]) for i, k in enumerate(kinds)}
    loads["dt"] = pltpu.make_async_copy(w_dt, wd.at[:, own_rows], load_sem.at[3])
    own_cols = pl.ds(pl.multiple_of(c * DB, DB), DB)
    sib_cols = pl.ds(pl.multiple_of((1 - c) * DB, DB), DB)
    loads["tok"] = pltpu.make_async_copy(tok_in, tok.at[x, :, own_cols], load_sem.at[4])
    wo_load = pltpu.make_async_copy(w_out, wo, load_sem.at[5])

    @pl.when(home)
    def _():
        for key in ("c", "dt", "tok", "g1", "g2"):
            loads[key].start()

    wo_load.start()

    barrier = pltpu.get_barrier_semaphore()
    peers = z_peers + y_peers + [plus, minus, sibling, halo_to, halo_from, swap]
    for peer in peers:
        pl.semaphore_signal(barrier, inc=1, device_id=peer, device_id_type=MESH)
    pl.semaphore_wait(barrier, len(peers))

    half = [pl.ds(0, HALF), pl.ds(HALF, HALF)]
    here = [(other, x * 2), (other, x * 2 + 1)]

    def fold(kind, index):
        push_if(home, w_in.at[:, cols_in(kind)], held[kind].at[own_rows, :], f_send.at[0, index], f_recv.at[0, index], sibling)
        for core in (0, 1):
            rows = pl.ds(64 * core, 64)
            there = pl.ds(pl.multiple_of(row_of(0, 0, 0) + 64 * core, 16), 64)
            push_if(
                away, w_in.at[rows, cols_in(kind)], held[kind].at[there, :],
                f_send.at[1 + core, index], f_recv.at[1, index], here[core],
            )

    def fold_dt():
        push_if(home, w_dt, wd.at[:, own_rows], f_send.at[0, 3], f_recv.at[0, 3], sibling)
        for core in (0, 1):
            push_if(away, w_dt, wd.at[:, own_rows], f_send.at[1 + core, 3], f_recv.at[1, 3], here[core])

    fold("c", 0)
    fold_dt()
    for k in (0, 1):
        rows = half[k]
        into = tok.at[x, rows, own_cols]
        push_if(away, tok_in.at[rows, :], into, t_send.at[14 + k], t_recv.at[14 + k], sibling)
        push_if(home, tok_in.at[rows, :], into, t_send.at[12 + k], t_recv.at[12 + k], (other, hd))
        push_if(away, tok_in.at[rows, :], into, t_send.at[12 + k], t_recv.at[14 + k], swap)
    fold("g1", 1)
    fold("g2", 2)

    def own_ready(kind, index):
        @pl.when(home)
        def _():
            loads[kind].wait()

        ref = wd.at[:, own_rows] if kind == "dt" else held[kind].at[own_rows, :]
        arrived_if(away, ref, f_recv.at[0, index])

    def partner_ready(kind, index):
        base = row_of(0, 0, 1)
        if kind == "dt":
            arrived(dt_block(0, 0, 1), f_recv.at[1, index])
        else:
            arrived(held[kind].at[pl.ds(pl.multiple_of(base + 64 * c, 16), 64), :], f_recv.at[1, index])

    def spread(stream, dy, dz):
        piece = block(stream, dy, dz, c)
        for a, b, d in children(stream, dy, dz):
            k = number(a, b)
            push(piece, piece, w_send.at[stream, k], w_recv.at[stream, k], target[d])
            if stream < 2:
                small = dt_block(dy, dz, stream)
                push(small, small, w_send.at[6 + stream, k], w_recv.at[6 + stream, k], target[d])
        if (dy, dz) != (0, 0) or STREAMS[stream][1]:
            k = number(dy, dz)
            push(piece, piece, d_send.at[stream, k], d_recv.at[stream, k], sibling)

    def all_here(streams):
        for stream in streams:
            for dy in (0, 1):
                for dz in range(NZ):
                    if (dy, dz) != (0, 0) or STREAMS[stream][1]:
                        arrived(block(stream, dy, dz, 1 - c), d_recv.at[stream, number(dy, dz)])

    def begin(stream):
        kind, partner = STREAMS[stream][:2]
        index = kinds.index(kind)
        if partner:
            partner_ready(kind, index)
            if stream == 1:
                partner_ready("dt", 3)
        else:
            own_ready(kind, index)
            if stream == 0:
                own_ready("dt", 3)
        spread(stream, 0, 0)

    def ring(stream, dy, dz):
        k = number(dy, dz)
        arrived(block(stream, dy, dz, c), w_recv.at[stream, k])
        if stream < 2:
            arrived(dt_block(dy, dz, stream), w_recv.at[6 + stream, k])
        spread(stream, dy, dz)

    def tok_piece(dx, k, p):
        return tok.at[lax.rem(x + dx + NX, NX), half[k], own_cols if p == 0 else sib_cols]

    def tok_spread(condition, k):
        for p in (0, 1):
            piece = tok_piece(0, k, p)
            push_if(condition, piece, piece, t_send.at[k * 2 + p], t_recv.at[k * 2 + p], plus)
        for p in (1, 0):
            piece = tok_piece(0, k, p)
            push_if(condition, piece, piece, t_send.at[4 + k * 2 + p], t_recv.at[4 + k * 2 + p], minus)

    def tok_in_home(k):
        if k == 0:
            pl.when(home)(loads["tok"].wait)
        arrived_if(home, tok_piece(0, k, 1), t_recv.at[14 + k])
        tok_spread(home, k)

    def tok_in_away(k):
        arrived_if(away, tok_piece(0, k, 0), t_recv.at[12 + k])
        arrived_if(away, tok_piece(0, k, 1), t_recv.at[14 + k])
        tok_spread(away, k)

    def tok_relay(dx, k, p):
        piece = tok_piece(dx, k, p)
        index = (0 if dx < 0 else 4) + k * 2 + p
        arrived(piece, t_recv.at[index])
        if dx < 0 and p == 0:
            push(piece, piece, t_send.at[8 + k], t_recv.at[8 + k], plus)
        if dx > 0 and p == 1:
            push(piece, piece, t_send.at[10 + k], t_recv.at[10 + k], minus)

    def tok_far(k, p):
        arrived(tok_piece(2, k, p), t_recv.at[(8 if p == 0 else 10) + k])

    def norm_rows(i, carry):
        rows = pl.ds(pl.multiple_of(i * 32, 32), 32)
        total = jnp.zeros((32, 1), F32)
        for h in range(8):
            v = tok[h // 2, rows, (h % 2) * DB : (h % 2 + 1) * DB].astype(F32)
            total = total + jnp.sum(v * v, axis=1, keepdims=True)
        scale = lax.rsqrt(total / (8 * DB) + EPS)
        for h in range(8):
            cols = slice((h % 2) * DB, (h % 2 + 1) * DB)
            v = tok[h // 2, rows, cols].astype(F32)
            xn[rows, h * DB : (h + 1) * DB] = (v * scale * norm_gain[:, h * DB : (h + 1) * DB]).astype(BF16)
        return carry

    def norm(i):
        lax.fori_loop(i * 3, i * 3 + 3, norm_rows, 0)

    def project(weights, first, width):
        cols = pl.ds(first, width)
        return jnp.dot(xn[...], weights[:, cols], preferred_element_type=F32).astype(BF16)

    def ship(buffer, tile, index):
        push_if(away, buffer.at[1, tile], buffer.at[0, tile], c_send.at[index], c_recv.at[index], swap)

    pending = []

    def channel_copies(tile):
        return (
            remote(halo_out.at[tile], halo_in.at[tile], h_send.at[tile], h_recv.at[tile], halo_to),
            remote(ch.at[1, tile], ch.at[0, tile], c_send.at[tile], c_recv.at[tile], swap),
        )

    def send_channels(tile):
        halo, rest = channel_copies(tile)
        halo.start()
        pl.when(away)(rest.start)

    def mats(second):
        def one(i, carry):
            tile = lax.rem(i + 4, 5)

            @pl.when(i > 0)
            def _():
                send_channels(lax.rem(i + 3, 5))

            value = project(wc, pl.multiple_of(tile * 256, 256), 256)
            ch[lent, tile] = value
            halo_out[tile] = value[ROWS - 16 :, :]
            return carry

        if second:
            value = project(wc, 512, 512)
            for tile in (2, 3):
                part_of = value[:, (tile - 2) * 256 : (tile - 1) * 256]
                ch[lent, tile] = part_of
                halo_out[tile] = part_of[ROWS - 16 :, :]
        else:
            lax.fori_loop(0, 3, one, 0)
        tiles = (2, 3) if second else (4, 0, 1)
        for tile in tiles:
            halo, rest = channel_copies(tile)
            sent.append(halo)
            sent_if.append((away, rest))

        def go():
            for tile in (2, 3) if second else (1,):
                send_channels(tile)

        pending.append(go)

    def dt():
        all_here((0, 1))
        raw[lent, 0] = dot_nt(wd[...], xn[...])
        pending.append(lambda: ship(raw, 0, 5))

    def gate_copy(tile):
        return remote(gs.at[1, tile], gs.at[0, tile], c_send.at[6 + tile], c_recv.at[6 + tile], swap)

    def gmats(second):
        all_here((4, 5) if second else (2, 3))
        base = 2 * second
        value = project(wg2 if second else wg1, 0, 512)
        for tile in (0, 1):
            gs[lent, base + tile] = value[:, tile * 256 : (tile + 1) * 256]
            sent_if.append((away, gate_copy(base + tile)))

        @pl.when(away)
        def _():
            gate_copy(base).start()
            gate_copy(base + 1).start()

    def chan(tile):
        arrived_if(away, ch.at[0, tile], c_recv.at[tile])
        chf[8:, tile * 256 : (tile + 1) * 256] = ch[0, tile].astype(F32)

    def column_of(ref):
        wide = jnp.concatenate([ref[...], jnp.zeros((1, 128 - NH), F32)], axis=1)
        return jnp.transpose(jnp.broadcast_to(wide, (128, 128)))[:NH, :1]

    row_id = lax.broadcasted_iota(jnp.int32, (128, 128), 0)
    lane_id = lax.broadcasted_iota(jnp.int32, (128, 128), 1)
    first_half = lane_id < 64
    upper_rows = row_id < 64

    def prep():
        arrived_if(away, raw.at[0, 0], c_recv.at[5])
        step = softplus(raw[0, 0] + column_of(dt_bias))
        decay = -jnp.exp(column_of(a_log)) * step
        upper = jnp.where(row_id <= lane_id, 1.0, 0.0).astype(F32)
        for q in range(CHUNKS):
            span = slice(q * 128, (q + 1) * 128)
            cum = jnp.dot(decay[:, span], upper, precision=HIGHEST, preferred_element_type=F32)
            to_end = jnp.exp(cum[:, 127:128] - cum) * step[:, span]
            ct[q] = cum
            stacked = jnp.concatenate(
                [cum, to_end, step[:, span], jnp.exp(cum), jnp.zeros((64, 128), F32)], axis=0
            )
            tt[q] = jnp.transpose(stacked)
        d_out[...] = jnp.broadcast_to(tt[0, 127:128, :] + tt[1, 127:128, :] + tt[2, 127:128, :], (8, 128))
        d_in[z] = d_out[...]

    def conv(tile):
        arrived(halo_in.at[tile], h_recv.at[tile])
        wide = slice(tile * 256, (tile + 1) * 256)
        chf[:8, wide] = jnp.where(s > 0, halo_in[tile, 8:16, :].astype(F32), 0.0)
        for cols in (slice(tile * 256, tile * 256 + 128), slice(tile * 256 + 128, tile * 256 + 256)):
            for q in range(CHUNKS):
                total = conv_b[:, cols] + jnp.zeros((128, 128), F32)
                for k in range(4):
                    total = total + conv_w[k, :, cols] * chf[q * 128 + 5 + k : q * 128 + 133 + k, cols]
                cv[q * 128 : (q + 1) * 128, cols] = silu(total).astype(BF16)

    def pair_cols(table, base, j):
        return jnp.where(
            first_half, table[:, base + 2 * j : base + 2 * j + 1], table[:, base + 2 * j + 1 : base + 2 * j + 2]
        )

    def pair_rows(row, j):
        return jnp.where(upper_rows, jnp.exp(row[:, 2 * j : 2 * j + 1]), jnp.exp(row[:, 2 * j + 1 : 2 * j + 2]))

    def end_states(tile):
        for j in (2 * tile, 2 * tile + 1):
            cols = slice(j * 128, (j + 1) * 128)
            for q in range(CHUNKS):
                span = slice(q * 128, (q + 1) * 128)
                weighted = (cv[span, cols].astype(F32) * pair_cols(tt[q], 16, j)).astype(BF16)
                fs[q, cols, :] = dot_tn(weighted, cv[span, 1024:1152])
            total = fs[1, cols, :] + pair_rows(tt[1, 127:128, :], j) * fs[0, cols, :]
            e_out[j] = (fs[2, cols, :] + pair_rows(tt[2, 127:128, :], j) * total).astype(BF16)

        def go():
            for j in (2 * tile, 2 * tile + 1):
                peer = (y * NZ + j, hd)
                push_if(z != j, e_out.at[j], e_in.at[z], s_send.at[0, j], s_recv.at[0, z], peer)
                push_if(z != j, d_out, d_in.at[z], s_send.at[1, j], s_recv.at[1, z], peer)

        pending.append(go)

    def inner(q, part_of):
        span = slice(q * 128, (q + 1) * 128)
        if part_of == 0:
            scores[...] = jnp.where(row_id >= lane_id, dot_nt(cv[span, 1152:1280], cv[span, 1024:1152]), 0.0)
        table = tt[q]
        for j in (2 * part_of, 2 * part_of + 1):
            cols = slice(j * 128, (j + 1) * 128)
            v = cv[span, cols].astype(F32)
            stepped = v * pair_cols(table, 32, j)
            values = jnp.concatenate(
                [jnp.where(first_half, stepped, 0.0), jnp.where(first_half, 0.0, stepped)], axis=0
            ).astype(BF16)
            weights = []
            for h in (2 * j, 2 * j + 1):
                gap = jnp.minimum(table[:, h : h + 1] - ct[q, h : h + 1, :], 0.0)
                weights.append((scores[...] * jnp.exp(gap)).astype(BF16))
            within = jnp.dot(jnp.concatenate(weights, axis=1), values, preferred_element_type=F32)
            skip = jnp.where(first_half[:1], d_skip[:, 2 * j : 2 * j + 1], d_skip[:, 2 * j + 1 : 2 * j + 2])
            ybuf[span, cols] = within + skip * v

    def ends():
        e_in[z] = e_out[z]

    lane_row = lax.broadcasted_iota(jnp.int32, (1, 128), 1)

    def pick(row, lane):
        return jnp.sum(jnp.where(lane_row == lane, row, 0.0), axis=1, keepdims=True)

    def factor(pair):
        return jnp.where(upper_rows[:, :1], jnp.exp(pair[0]), jnp.exp(pair[1]))

    before = []

    def prefix():
        for k in range(1, NZ):
            source = lax.rem(z + NZ - k, NZ)
            arrived(e_in.at[source], s_recv.at[0, source])
            arrived(d_in.at[source], s_recv.at[1, source])
        running = jnp.zeros((128, 128), F32)
        gone = (jnp.zeros((1, 1), F32), jnp.zeros((1, 1), F32))
        for k in range(NZ):
            pre[k] = running
            before.append(gone)
            row = d_in[k, :1, :]
            pair = (pick(row, 2 * z), pick(row, 2 * z + 1))
            running = factor(pair) * running + e_in[k].astype(F32)
            gone = (gone[0] + pair[0], gone[1] + pair[1])
        row_out[...] = running.astype(BF16)
        rowd_out[...] = jnp.broadcast_to(jnp.where(lane_row == 0, gone[0], gone[1]), (8, 128))
        row_in[y] = running.astype(BF16)
        rowd_in[y] = jnp.broadcast_to(jnp.where(lane_row == 0, gone[0], gone[1]), (8, 128))

        def go():
            for k in range(1, NY):
                push(row_out, row_in.at[y], r_send.at[0, k], r_recv.at[0, k], y_peers[k - 1])
                push(rowd_out, rowd_in.at[y], r_send.at[1, k], r_recv.at[1, k], y_peers[k - 1])

        pending.append(go)

    def back():
        for k in range(1, NY):
            source = lax.rem(y + NY - k, NY)
            arrived(row_in.at[source], r_recv.at[0, k])
            arrived(rowd_in.at[source], r_recv.at[1, k])
        entering = jnp.zeros((128, 128), F32)
        for k in range(NY):
            row = rowd_in[k, :1, :]
            moved = factor((row[:, 0:1], row[:, 1:2])) * entering + row_in[k].astype(F32)
            entering = jnp.where(k < y, moved, entering)
        for k in range(NZ):
            back_out[k] = (factor(before[k]) * entering + pre[k]).astype(BF16)
        sin[z] = back_out[z]

        def go():
            for k in range(1, NZ):
                peer = lax.rem(z + k, NZ)
                push(back_out.at[peer], sin.at[z], b_send.at[k], b_recv.at[k], z_peers[k - 1])

        pending.append(go)

    def carry():
        for k in range(1, NZ):
            arrived(sin.at[lax.rem(z + NZ - k, NZ)], b_recv.at[k])
        for j in range(8):
            cols = slice(j * 128, (j + 1) * 128)
            entering = sin[j].astype(F32)
            for q in range(CHUNKS):
                span = slice(q * 128, (q + 1) * 128)
                across = dot_nt(cv[span, 1152:1280], entering.astype(BF16))
                ybuf[span, cols] += pair_cols(tt[q], 48, j) * across
                if q < CHUNKS - 1:
                    entering = pair_rows(tt[q, 127:128, :], j) * entering + fs[q, cols, :]

    squares = [jnp.zeros((ROWS, 1), F32)]

    def gate(tile):
        cols = slice(tile * 256, (tile + 1) * 256)
        arrived_if(away, gs.at[0, tile], c_recv.at[6 + tile])
        gated = ybuf[:, cols] * silu(gs[0, tile].astype(F32))
        ybuf[:, cols] = gated
        squares[0] = squares[0] + jnp.sum(gated * gated, axis=1, keepdims=True)

    steps = {
        "begin": begin, "ring": ring, "tinh": tok_in_home, "tin": tok_in_away, "tr": tok_relay, "ta": tok_far, "norm": norm, "mats": mats,
        "dt": dt, "gmats": gmats, "chan": chan, "prep": prep, "conv": conv, "state": end_states, "inner": inner,
        "ends": ends, "prefix": prefix, "back": back, "carry": carry, "gate": gate,
    }
    for step in PLAN:
        later, pending[:] = list(pending), []
        for go in later:
            go()
        steps[step[0]](*step[1:])
    for go in pending:
        go()
    scale = lax.rsqrt(squares[0] / GC + EPS)

    def norm_tile(i, carry):
        cols = pl.ds(pl.multiple_of(i * 128, 128), 128)
        no[:, cols] = (ybuf[:, cols] * scale * gate_gain[:, cols]).astype(BF16)
        return carry

    lax.fori_loop(0, 8, norm_tile, 0)
    wo_load.wait()

    def term(dx, core, into, rows=slice(None)):
        cols = pl.ds(pl.multiple_of(head_of(dx, core) * DB, DB), DB)
        into[...] = jnp.dot(no[rows, :], wo[:, cols], preferred_element_type=F32).astype(into.dtype)

    top, low = half

    def to_sibling(r):
        term(r, 1 - c, sib_out.at[r])

    def keep(r):
        term(r, c, part.at[r])

    def send_sibling(r):
        push(sib_out.at[r], sib_in.at[r], o_send.at[r], o_recv.at[r], sibling)

    def chip_sum(r, rows):
        return part[r, rows, :] + sib_in[r, rows, :].astype(F32)

    for k, rows in enumerate(half):
        term(2, 1 - c, sib_out.at[2, rows, :], rows)
        term(2, c, part.at[2, rows, :], rows)
        push(sib_out.at[2, rows, :], sib_in.at[2, rows, :], o_send.at[2 + 2 * k], o_recv.at[2 + 2 * k], sibling)
    to_sibling(1)
    arrived(sib_in.at[2, top, :], o_recv.at[2])
    far_out[top, :] = chip_sum(2, top).astype(BF16)
    arrived(sib_in.at[2, low, :], o_recv.at[4])
    far_out[low, :] = chip_sum(2, low).astype(BF16)
    push(far_out.at[top, :], far_in.at[0], x_send.at[0], x_recv.at[0], plus)
    send_sibling(1)
    to_sibling(3)
    push(far_out.at[low, :], far_in.at[1], x_send.at[1], x_recv.at[1], minus)
    keep(1)
    send_sibling(3)
    keep(3)
    arrived(sib_in.at[1], o_recv.at[1])
    near_out[0, low, :] = chip_sum(1, low).astype(BF16)
    arrived(sib_in.at[3], o_recv.at[3])
    near_out[1, top, :] = chip_sum(3, top).astype(BF16)
    push(near_out.at[0, low, :], near_in.at[0, low, :], x_send.at[2], x_recv.at[2], plus)
    to_sibling(0)
    push(near_out.at[1, top, :], near_in.at[1, top, :], x_send.at[3], x_recv.at[3], minus)
    keep(0)
    send_sibling(0)
    arrived(far_in.at[0], x_recv.at[0])
    near_out[0, top, :] = (chip_sum(1, top) + far_in[0].astype(F32)).astype(BF16)
    push(near_out.at[0, top, :], near_in.at[0, top, :], x_send.at[4], x_recv.at[4], plus)
    arrived(far_in.at[1], x_recv.at[1])
    near_out[1, low, :] = (chip_sum(3, low) + far_in[1].astype(F32)).astype(BF16)
    push(near_out.at[1, low, :], near_in.at[1, low, :], x_send.at[5], x_recv.at[5], minus)
    arrived(sib_in.at[0], o_recv.at[0])
    part[0] = chip_sum(0, slice(None))
    arrived(near_in.at[0, low, :], x_recv.at[2])
    arrived(near_in.at[1, top, :], x_recv.at[3])
    arrived(near_in.at[0, top, :], x_recv.at[4])
    arrived(near_in.at[1, low, :], x_recv.at[5])
    out_ref[...] = (part[0] + near_in[0].astype(F32) + near_in[1].astype(F32)).astype(BF16)
    for copy in sent:
        copy.wait_send()
    for condition, copy in sent_if:
        pl.when(condition)(copy.wait_send)


def body(tokens, norm_gain, w_in, w_dt, dt_bias, a_log, d_skip, conv_w, conv_b, gate_gain, w_out):
    any_space = pl.BlockSpec(memory_space=pl.ANY)
    vmem = pl.BlockSpec(memory_space=pltpu.VMEM)
    dma = pltpu.SemaphoreType.DMA

    def buf(*shape, dtype=BF16):
        return pltpu.VMEM(shape, dtype)

    scratch = [
        buf(NX, ROWS, 2 * DB), buf(ROWS, 4096), buf(4096, CC), buf(4096, G1), buf(4096, G2),
        buf(NH, 4096), buf(GC, 4096), buf(2, 5, ROWS, 256), buf(2, 4, ROWS, 256),
        buf(2, 1, NH, ROWS, dtype=F32),
        buf(ROWS + 8, CC, dtype=F32), buf(5, 16, 256), buf(5, 16, 256), buf(ROWS, CC), buf(ROWS, GC, dtype=F32),
        buf(CHUNKS, 128, 128, dtype=F32), buf(CHUNKS, NH, 128, dtype=F32), buf(CHUNKS, GC, 128, dtype=F32), buf(128, 128, dtype=F32),
        buf(8, 128, 128), buf(8, 128, dtype=F32), buf(8, 128, 128), buf(8, 8, 128, dtype=F32),
        buf(8, 128, 128, dtype=F32),
        buf(128, 128), buf(8, 128, dtype=F32), buf(NY, 128, 128), buf(NY, 8, 128, dtype=F32),
        buf(8, 128, 128), buf(8, 128, 128),
        buf(ROWS, GC), buf(4, ROWS, DB), buf(4, ROWS, DB), buf(4, ROWS, DB, dtype=F32),
        buf(ROWS, DB), buf(2, ROWS // 2, DB), buf(2, ROWS, DB), buf(2, ROWS, DB),
        dma((6,)), dma((8, 16)), dma((8, 16)), dma((3, 4)), dma((2, 4)), dma((6, 16)), dma((6, 16)),
        dma((16,)), dma((16,)), dma((10,)), dma((10,)), dma((5,)), dma((5,)),
        dma((2, NZ)), dma((2, NZ)), dma((2, NY)), dma((2, NY)), dma((NZ,)), dma((NZ,)),
        dma((5,)), dma((5,)), dma((6,)), dma((6,)),
    ]
    return pl.pallas_call(
        kernel,
        out_shape=jax.ShapeDtypeStruct((ROWS, DB), BF16),
        in_specs=[any_space] * 4 + [vmem] * 7,
        out_specs=vmem,
        scratch_shapes=scratch,
        compiler_params=pltpu.CompilerParams(
            collective_id=0, has_side_effects=True, vmem_limit_bytes=64 * 1024 * 1024 - 65536
        ),
    )(
        tokens, w_in.reshape(SUB, GC + CC), w_dt.T, w_out.reshape(GC, 4096),
        norm_gain.reshape(1, 4096), dt_bias.reshape(1, NH), a_log.reshape(1, NH), d_skip.reshape(1, NH),
        conv_w, conv_b, gate_gain,
    )


def solution(mesh):
    in_specs = (
        P("seq", "head"), P(), P("seq", "head", None), P("seq", "head"), P("head"), P("head"), P("head"),
        P(None, "head", None), P("head", None), P("head", None), P("head", None, None),
    )
    return jax.shard_map(body, mesh=mesh, in_specs=in_specs, out_specs=P("seq", "head"), check_vma=False)
```

```python
import heapq
import itertools

import jax
import jax.numpy as jnp
from jax import lax
from jax.experimental import pallas as pl
from jax.experimental.pallas import tpu as pltpu
from jax.sharding import PartitionSpec as P

EPS = 1e-05
HIGHEST = lax.Precision.HIGHEST
MESH = pl.DeviceIdType.MESH
F32 = jnp.float32
BF16 = jnp.bfloat16

NY, NZ, NX = 4, 8, 4
ROWS = 384
HALF = ROWS // 2
DB = 512
SUB = 128
CC = 1280
GC = 1024
G1, G2 = 512, 512
NH = 16
CHUNKS = 3

STREAMS = (
    ("c", 0, 0, 64, True),
    ("c", 1, 0, 64, False),
    ("g1", 0, 0, 64, True),
    ("g1", 1, 0, 64, True),
    ("g2", 0, 0, 64, True),
    ("g2", 1, 0, 64, False),
)
WIDTH = {"c": CC, "g1": G1, "g2": G2}
FIRST = {"c": GC, "g1": 0, "g2": G1}


def children(stream, dy, dz):
    along_z, flip = STREAMS[stream][4], stream in (2, 3)
    out = []
    if along_z:
        up, down = (3, 4) if flip else (4, 3)
        if dy == 0:
            if 0 <= dz < up:
                out.append((0, dz + 1, "z+"))
            if 0 <= -dz < down:
                out.append((0, dz - 1, "z-"))
            out.append((1, dz, "y"))
    else:
        if (dy, dz) == (0, 0):
            out.append((1, 0, "y"))
        up, down = (4, 3) if (dy == 0) != flip else (3, 4)
        if 0 <= dz < up:
            out.append((dy, dz + 1, "z+"))
        if 0 <= -dz < down:
            out.append((dy, dz - 1, "z-"))
    return out


STARTS = {26: (2, 3), 32: (4, 5)}
EX, HAND = (1.0, 3.5, 1.0), {"c": 1.5, "g1": 3.0, "g2": 3.0}
TIN, FOLD, XRATE = (12.0, 14.0), 10.0, (80000.0, 45000.0)


def plan():
    free = dict.fromkeys(("y", "z+", "z-", "x+", "x-"), 0.0)
    events, done, order, tick = [], {}, [], itertools.count()
    left = {"c": 30, "g1": 30, "g2": 30, "tok": 12}
    taken = {"ring": 0}
    rate = 45000.0

    def later(t, item):
        heapq.heappush(events, (t, next(tick), item))

    def send(t, link, size, item, speed=45000.0):
        free[link] = max(t, free[link]) + size / speed
        later(free[link] + 2.2, item)

    def ring(t, stream, dy, dz):
        kind, _, _, rows, _ = STREAMS[stream]
        for a, b, d in children(stream, dy, dz):
            send(t, d, rows * WIDTH[kind] * 2, ("ring", stream, a, b))

    piece = HALF * DB * 2
    for item, t in ((("tinh", 0), 3.0), (("tinh", 1), 3.5), (("tin", 0), TIN[0]), (("tin", 1), TIN[1]), (("own", 0), 1.5), (("fold", 1), FOLD)):
        later(t, item)
    fold_at = {"g1": 20.0, "g2": 21.0}

    tiles = (4, 0, 1, 2, 3)
    units = [(("norm", i), 0.65, [("tok",)] if i == 0 else [("norm", i - 1)]) for i in range(4)]
    units += [(("prefix",), 0.4, [("ex1",)]), (("back",), 0.4, [("ex2",)])]
    units += [(("ends",), 0.2, [("state", i) for i in range(4)])]
    units += [(("dt",), 1.2, [("c",), ("norm", 3)]), (("mats", 0), 3.6, [("dt",)]), (("mats", 1), 1.9, [("mats", 0)])]
    units += [(("state", i), 0.7, [("conv", i), ("conv", 4), ("prep",)]) for i in range(4)]
    units += [(("conv", i), 0.5, [("halo", i), ("chan", i)]) for i in tiles]
    units += [(("chan", i), 0.1, [("ch", i)]) for i in tiles]
    units += [(("prep",), 0.8, [("raw",)])]
    units += [(("carry",), 1.4, [("ex3",)] + [("inner", q, j) for q in range(CHUNKS) for j in range(4)])]
    units += [(("gate", i), 0.35, [("carry",), ("g", i)]) for i in range(4)]
    units += [(("gmats", 0), 1.9, [("g1",), ("mats", 1)]), (("gmats", 1), 1.9, [("g2",), ("mats", 1)])]
    units += [(("inner", q, j), 0.45, [("state", i) for i in range(4)]) for q in range(CHUNKS) for j in range(4)]

    now = 0.0
    while events or units:
        ready = [e for e in events if e[0] <= now]
        if ready:
            e = min(ready)
            events.remove(e)
            item = e[2]
            if item[0] == "ring":
                order.append(item)
                stream = item[1]
                kind = STREAMS[stream][0]
                left[kind] -= 1
                if not left[kind]:
                    later(now + HAND[kind], ("flag", (kind,)))
                ring(now, *item[1:])
                taken["ring"] += 1
                for late in STARTS.get(taken["ring"], ()):
                    order.append(("begin", late))
                    ring(max(now, fold_at[STREAMS[late][0]]), late, 0, 0)
            elif item[0] in ("own", "fold"):
                order.append(("begin", item[1]))
                ring(now, item[1], 0, 0)
            elif item[0] == "tinh":
                order.append(item)
            elif item[0] == "tin":
                order.append(item)
                k = item[1]
                for p in (0, 1):
                    send(now, "x+", piece, ("tr", -1, k, p), XRATE[0])
                for p in (1, 0):
                    send(now, "x-", piece, ("tr", 1, k, p), XRATE[0])
            elif item[0] == "tr":
                order.append(item)
                _, dx, k, p = item
                if dx < 0 and p == 0:
                    send(now, "x+", piece, ("ta", k, p), XRATE[1])
                if dx > 0 and p == 1:
                    send(now, "x-", piece, ("ta", k, p), XRATE[1])
                left["tok"] -= 1
            elif item[0] == "ta":
                order.append(item)
                left["tok"] -= 1
            elif item[0] == "flag":
                done[item[1]] = now
            if item[0] in ("tr", "ta") and not left["tok"]:
                done[("tok",)] = now
            now += 0.05
            continue
        todo = [u for u in units if all(n in done for n in u[2])]
        if todo:
            unit = todo[0]
            units.remove(unit)
            name = unit[0]
            order.append(name)
            now += unit[1]
            done[name] = now
            if name[0] == "mats":
                for i, tile in enumerate((2, 3) if name[1] else (4, 0, 1)):
                    wait = 3.0 + 1.8 * i if name[1] else 2.0 + i
                    later(now + wait, ("flag", ("ch", tile)))
                    later(now + wait + 0.5, ("flag", ("halo", tile)))
            if name[0] == "dt":
                later(now + 2.5, ("flag", ("raw",)))
            if name[0] == "gmats":
                for i in (0, 1):
                    later(now + 4.5, ("flag", ("g", 2 * name[1] + i)))
            if name[0] in ("state", "back"):
                size = 74000 if name[0] == "state" else 295000
                for link in ("z+", "z-"):
                    free[link] = max(now, free[link]) + size / rate
                if name[0] == "back":
                    later(max(free["z+"], free["z-"]) + EX[2], ("flag", ("ex3",)))
            if name[0] == "ends":
                later(max(free["z+"], free["z-"], now) + EX[0], ("flag", ("ex1",)))
            if name[0] == "prefix":
                later(now + EX[1], ("flag", ("ex2",)))
            continue
        if not events:
            raise ValueError("stuck")
        now = min(events)[0]
    return order


PLAN = plan()


def number(dy, dz):
    return dy * NZ + dz % NZ


def softplus(v):
    return jnp.maximum(v, 0.0) + jnp.log1p(jnp.exp(-jnp.abs(v)))


def silu(v):
    return v / (1.0 + jnp.exp(-v))


def dot_nt(a, b):
    return lax.dot_general(a, b, (((1,), (1,)), ((), ())), preferred_element_type=F32)


def dot_tn(a, b):
    return lax.dot_general(a, b, (((0,), (0,)), ((), ())), preferred_element_type=F32)


def kernel(
    tok_in, w_in, w_dt, w_out, norm_gain, dt_bias, a_log, d_skip, conv_w, conv_b, gate_gain,
    out_ref,
    tok, xn, wc, wg1, wg2, wd, wo, ch, gs, raw,
    chf, halo_out, halo_in, cv, ybuf, tt, ct, fs, scores,
    e_out, d_out, e_in, d_in, pre, row_out, rowd_out, row_in, rowd_in, back_out, sin,
    no, sib_out, sib_in, part, far_out, far_in, near_out, near_in,
    load_sem, w_send, w_recv, f_send, f_recv, d_send, d_recv, t_send, t_recv, c_send, c_recv, h_send, h_recv,
    s_send, s_recv, r_send, r_recv, b_send, b_recv, o_send, o_recv, x_send, x_recv,
):
    s = lax.axis_index("seq")
    hd = lax.axis_index("head")
    y, z = lax.div(s, NZ), lax.rem(s, NZ)
    x, c = lax.div(hd, 2), lax.rem(hd, 2)
    kind_of_row = lax.div(y, 2)
    home = c == kind_of_row
    away = c != kind_of_row

    def at_yz(dy, dz):
        return lax.rem(y + dy + 2 * NY, NY) * NZ + lax.rem(z + dz + 2 * NZ, NZ)

    def head_of(dx, core):
        return lax.rem(x + dx + NX, NX) * 2 + core

    other = (NY - 1 - y) * NZ + z
    mate = (y + 1 - 2 * lax.rem(y, 2)) * NZ + z
    sibling = (s, x * 2 + (1 - c))
    plus, minus = (s, head_of(1, c)), (s, head_of(-1, c))
    lent = lax.select(home, 0, 1)
    halo_to = (lax.rem(lax.select(home, s, other) + 1, NY * NZ), x * 2 + lax.select(home, c, 1 - c))
    earlier = lax.rem(s + NY * NZ - 1, NY * NZ)
    earlier_row = lax.div(earlier, NZ)
    earlier_home = lax.div(earlier_row, 2) == c
    halo_from = (
        lax.select(earlier_home, earlier, (NY - 1 - earlier_row) * NZ + lax.rem(earlier, NZ)),
        x * 2 + lax.select(earlier_home, c, 1 - c),
    )
    target = {"y": (mate, hd), "z+": (at_yz(0, 1), hd), "z-": (at_yz(0, -1), hd)}
    z_peers = [(at_yz(0, k), hd) for k in range(1, NZ)]
    y_peers = [(at_yz(k, 0), hd) for k in range(1, NY)]
    swap = (other, x * 2 + (1 - c))
    sent, sent_if = [], []

    def remote(src, dst, send, recv, where):
        return pltpu.make_async_remote_copy(
            src_ref=src, dst_ref=dst, send_sem=send, recv_sem=recv, device_id=where, device_id_type=MESH
        )

    def push(src, dst, send, recv, where):
        copy = remote(src, dst, send, recv, where)
        copy.start()
        sent.append(copy)

    def push_if(condition, src, dst, send, recv, where):
        copy = remote(src, dst, send, recv, where)
        pl.when(condition)(copy.start)
        sent_if.append((condition, copy))

    def arrived(ref, recv):
        remote(ref, ref, recv, recv, sibling).wait_recv()

    def arrived_if(condition, ref, recv):
        pl.when(condition)(remote(ref, ref, recv, recv, sibling).wait_recv)

    held = {"c": wc, "g1": wg1, "g2": wg2}

    def cols_in(kind):
        return pl.ds(FIRST[kind], WIDTH[kind])

    def row_of(dy, dz, partner):
        row = y + dy * (1 - 2 * lax.rem(y, 2))
        row = NY - 1 - row if partner else row
        return (row * NZ + lax.rem(z - dz + NZ, NZ)) * SUB

    def block(stream, dy, dz, core):
        kind, partner, first, rows, _ = STREAMS[stream]
        base = row_of(dy, dz, partner) + 64 * core + first
        return held[kind].at[pl.ds(pl.multiple_of(base, 16), rows), :]

    def dt_block(dy, dz, partner):
        return wd.at[:, pl.ds(pl.multiple_of(row_of(dy, dz, partner), SUB), SUB)]

    own_rows = pl.ds(pl.multiple_of(row_of(0, 0, 0), SUB), SUB)
    kinds = ("c", "g1", "g2")
    loads = {k: pltpu.make_async_copy(w_in.at[:, cols_in(k)], held[k].at[own_rows, :], load_sem.at[i]) for i, k in enumerate(kinds)}
    loads["dt"] = pltpu.make_async_copy(w_dt, wd.at[:, own_rows], load_sem.at[3])
    own_cols = pl.ds(pl.multiple_of(c * DB, DB), DB)
    sib_cols = pl.ds(pl.multiple_of((1 - c) * DB, DB), DB)
    loads["tok"] = pltpu.make_async_copy(tok_in, tok.at[x, :, own_cols], load_sem.at[4])
    wo_load = pltpu.make_async_copy(w_out, wo, load_sem.at[5])

    @pl.when(home)
    def _():
        for key in ("c", "dt", "tok", "g1", "g2"):
            loads[key].start()

    wo_load.start()

    barrier = pltpu.get_barrier_semaphore()
    peers = z_peers + y_peers + [plus, minus, sibling, halo_to, halo_from, swap]
    for peer in peers:
        pl.semaphore_signal(barrier, inc=1, device_id=peer, device_id_type=MESH)
    pl.semaphore_wait(barrier, len(peers))

    half = [pl.ds(0, HALF), pl.ds(HALF, HALF)]
    here = [(other, x * 2), (other, x * 2 + 1)]

    def fold(kind, index):
        push_if(home, w_in.at[:, cols_in(kind)], held[kind].at[own_rows, :], f_send.at[0, index], f_recv.at[0, index], sibling)
        for core in (0, 1):
            rows = pl.ds(64 * core, 64)
            there = pl.ds(pl.multiple_of(row_of(0, 0, 0) + 64 * core, 16), 64)
            push_if(
                away, w_in.at[rows, cols_in(kind)], held[kind].at[there, :],
                f_send.at[1 + core, index], f_recv.at[1, index], here[core],
            )

    def fold_dt():
        push_if(home, w_dt, wd.at[:, own_rows], f_send.at[0, 3], f_recv.at[0, 3], sibling)
        for core in (0, 1):
            push_if(away, w_dt, wd.at[:, own_rows], f_send.at[1 + core, 3], f_recv.at[1, 3], here[core])

    fold("c", 0)
    fold_dt()
    for k in (0, 1):
        rows = half[k]
        into = tok.at[x, rows, own_cols]
        push_if(away, tok_in.at[rows, :], into, t_send.at[14 + k], t_recv.at[14 + k], sibling)
        push_if(home, tok_in.at[rows, :], into, t_send.at[12 + k], t_recv.at[12 + k], (other, hd))
        push_if(away, tok_in.at[rows, :], into, t_send.at[12 + k], t_recv.at[14 + k], swap)
    fold("g1", 1)
    fold("g2", 2)

    def own_ready(kind, index):
        @pl.when(home)
        def _():
            loads[kind].wait()

        ref = wd.at[:, own_rows] if kind == "dt" else held[kind].at[own_rows, :]
        arrived_if(away, ref, f_recv.at[0, index])

    def partner_ready(kind, index):
        base = row_of(0, 0, 1)
        if kind == "dt":
            arrived(dt_block(0, 0, 1), f_recv.at[1, index])
        else:
            arrived(held[kind].at[pl.ds(pl.multiple_of(base + 64 * c, 16), 64), :], f_recv.at[1, index])

    def spread(stream, dy, dz):
        piece = block(stream, dy, dz, c)
        for a, b, d in children(stream, dy, dz):
            k = number(a, b)
            push(piece, piece, w_send.at[stream, k], w_recv.at[stream, k], target[d])
            if stream < 2:
                small = dt_block(dy, dz, stream)
                push(small, small, w_send.at[6 + stream, k], w_recv.at[6 + stream, k], target[d])
        if (dy, dz) != (0, 0) or STREAMS[stream][1]:
            k = number(dy, dz)
            push(piece, piece, d_send.at[stream, k], d_recv.at[stream, k], sibling)

    def all_here(streams):
        for stream in streams:
            for dy in (0, 1):
                for dz in range(NZ):
                    if (dy, dz) != (0, 0) or STREAMS[stream][1]:
                        arrived(block(stream, dy, dz, 1 - c), d_recv.at[stream, number(dy, dz)])

    def begin(stream):
        kind, partner = STREAMS[stream][:2]
        index = kinds.index(kind)
        if partner:
            partner_ready(kind, index)
            if stream == 1:
                partner_ready("dt", 3)
        else:
            own_ready(kind, index)
            if stream == 0:
                own_ready("dt", 3)
        spread(stream, 0, 0)

    def ring(stream, dy, dz):
        k = number(dy, dz)
        arrived(block(stream, dy, dz, c), w_recv.at[stream, k])
        if stream < 2:
            arrived(dt_block(dy, dz, stream), w_recv.at[6 + stream, k])
        spread(stream, dy, dz)

    def tok_piece(dx, k, p):
        return tok.at[lax.rem(x + dx + NX, NX), half[k], own_cols if p == 0 else sib_cols]

    def tok_spread(condition, k):
        for p in (0, 1):
            piece = tok_piece(0, k, p)
            push_if(condition, piece, piece, t_send.at[k * 2 + p], t_recv.at[k * 2 + p], plus)
        for p in (1, 0):
            piece = tok_piece(0, k, p)
            push_if(condition, piece, piece, t_send.at[4 + k * 2 + p], t_recv.at[4 + k * 2 + p], minus)

    def tok_in_home(k):
        if k == 0:
            pl.when(home)(loads["tok"].wait)
        arrived_if(home, tok_piece(0, k, 1), t_recv.at[14 + k])
        tok_spread(home, k)

    def tok_in_away(k):
        arrived_if(away, tok_piece(0, k, 0), t_recv.at[12 + k])
        arrived_if(away, tok_piece(0, k, 1), t_recv.at[14 + k])
        tok_spread(away, k)

    def tok_relay(dx, k, p):
        piece = tok_piece(dx, k, p)
        index = (0 if dx < 0 else 4) + k * 2 + p
        arrived(piece, t_recv.at[index])
        if dx < 0 and p == 0:
            push(piece, piece, t_send.at[8 + k], t_recv.at[8 + k], plus)
        if dx > 0 and p == 1:
            push(piece, piece, t_send.at[10 + k], t_recv.at[10 + k], minus)

    def tok_far(k, p):
        arrived(tok_piece(2, k, p), t_recv.at[(8 if p == 0 else 10) + k])

    def norm_rows(i, carry):
        rows = pl.ds(pl.multiple_of(i * 32, 32), 32)
        total = jnp.zeros((32, 1), F32)
        for h in range(8):
            v = tok[h // 2, rows, (h % 2) * DB : (h % 2 + 1) * DB].astype(F32)
            total = total + jnp.sum(v * v, axis=1, keepdims=True)
        scale = lax.rsqrt(total / (8 * DB) + EPS)
        for h in range(8):
            cols = slice((h % 2) * DB, (h % 2 + 1) * DB)
            v = tok[h // 2, rows, cols].astype(F32)
            xn[rows, h * DB : (h + 1) * DB] = (v * scale * norm_gain[:, h * DB : (h + 1) * DB]).astype(BF16)
        return carry

    def norm(i):
        lax.fori_loop(i * 3, i * 3 + 3, norm_rows, 0)

    def project(weights, first, width):
        cols = pl.ds(first, width)
        return jnp.dot(xn[...], weights[:, cols], preferred_element_type=F32).astype(BF16)

    def ship(buffer, tile, index):
        push_if(away, buffer.at[1, tile], buffer.at[0, tile], c_send.at[index], c_recv.at[index], swap)

    pending = []

    def channel_copies(tile):
        return (
            remote(halo_out.at[tile], halo_in.at[tile], h_send.at[tile], h_recv.at[tile], halo_to),
            remote(ch.at[1, tile], ch.at[0, tile], c_send.at[tile], c_recv.at[tile], swap),
        )

    def send_channels(tile):
        halo, rest = channel_copies(tile)
        halo.start()
        pl.when(away)(rest.start)

    def mats(second):
        def one(i, carry):
            tile = lax.rem(i + 4, 5)

            @pl.when(i > 0)
            def _():
                send_channels(lax.rem(i + 3, 5))

            value = project(wc, pl.multiple_of(tile * 256, 256), 256)
            ch[lent, tile] = value
            halo_out[tile] = value[ROWS - 16 :, :]
            return carry

        if second:
            value = project(wc, 512, 512)
            for tile in (2, 3):
                part_of = value[:, (tile - 2) * 256 : (tile - 1) * 256]
                ch[lent, tile] = part_of
                halo_out[tile] = part_of[ROWS - 16 :, :]
        else:
            lax.fori_loop(0, 3, one, 0)
        tiles = (2, 3) if second else (4, 0, 1)
        for tile in tiles:
            halo, rest = channel_copies(tile)
            sent.append(halo)
            sent_if.append((away, rest))

        def go():
            for tile in (2, 3) if second else (1,):
                send_channels(tile)

        pending.append(go)

    def dt():
        all_here((0, 1))
        raw[lent, 0] = dot_nt(wd[...], xn[...])
        pending.append(lambda: ship(raw, 0, 5))

    def gate_copy(tile):
        return remote(gs.at[1, tile], gs.at[0, tile], c_send.at[6 + tile], c_recv.at[6 + tile], swap)

    def gmats(second):
        all_here((4, 5) if second else (2, 3))
        base = 2 * second
        value = project(wg2 if second else wg1, 0, 512)
        for tile in (0, 1):
            gs[lent, base + tile] = value[:, tile * 256 : (tile + 1) * 256]
            sent_if.append((away, gate_copy(base + tile)))

        @pl.when(away)
        def _():
            gate_copy(base).start()
            gate_copy(base + 1).start()

    def chan(tile):
        arrived_if(away, ch.at[0, tile], c_recv.at[tile])
        chf[8:, tile * 256 : (tile + 1) * 256] = ch[0, tile].astype(F32)

    def column_of(ref):
        wide = jnp.concatenate([ref[...], jnp.zeros((1, 128 - NH), F32)], axis=1)
        return jnp.transpose(jnp.broadcast_to(wide, (128, 128)))[:NH, :1]

    row_id = lax.broadcasted_iota(jnp.int32, (128, 128), 0)
    lane_id = lax.broadcasted_iota(jnp.int32, (128, 128), 1)
    first_half = lane_id < 64
    upper_rows = row_id < 64

    def prep():
        arrived_if(away, raw.at[0, 0], c_recv.at[5])
        step = softplus(raw[0, 0] + column_of(dt_bias))
        decay = -jnp.exp(column_of(a_log)) * step
        upper = jnp.where(row_id <= lane_id, 1.0, 0.0).astype(F32)
        for q in range(CHUNKS):
            span = slice(q * 128, (q + 1) * 128)
            cum = jnp.dot(decay[:, span], upper, precision=HIGHEST, preferred_element_type=F32)
            to_end = jnp.exp(cum[:, 127:128] - cum) * step[:, span]
            ct[q] = cum
            stacked = jnp.concatenate(
                [cum, to_end, step[:, span], jnp.exp(cum), jnp.zeros((64, 128), F32)], axis=0
            )
            tt[q] = jnp.transpose(stacked)
        d_out[...] = jnp.broadcast_to(tt[0, 127:128, :] + tt[1, 127:128, :] + tt[2, 127:128, :], (8, 128))
        d_in[z] = d_out[...]

    def conv(tile):
        arrived(halo_in.at[tile], h_recv.at[tile])
        wide = slice(tile * 256, (tile + 1) * 256)
        chf[:8, wide] = jnp.where(s > 0, halo_in[tile, 8:16, :].astype(F32), 0.0)
        for cols in (slice(tile * 256, tile * 256 + 128), slice(tile * 256 + 128, tile * 256 + 256)):
            for q in range(CHUNKS):
                total = conv_b[:, cols] + jnp.zeros((128, 128), F32)
                for k in range(4):
                    total = total + conv_w[k, :, cols] * chf[q * 128 + 5 + k : q * 128 + 133 + k, cols]
                cv[q * 128 : (q + 1) * 128, cols] = silu(total).astype(BF16)

    def pair_cols(table, base, j):
        return jnp.where(
            first_half, table[:, base + 2 * j : base + 2 * j + 1], table[:, base + 2 * j + 1 : base + 2 * j + 2]
        )

    def pair_rows(row, j):
        return jnp.where(upper_rows, jnp.exp(row[:, 2 * j : 2 * j + 1]), jnp.exp(row[:, 2 * j + 1 : 2 * j + 2]))

    def end_states(tile):
        for j in (2 * tile, 2 * tile + 1):
            cols = slice(j * 128, (j + 1) * 128)
            for q in range(CHUNKS):
                span = slice(q * 128, (q + 1) * 128)
                weighted = (cv[span, cols].astype(F32) * pair_cols(tt[q], 16, j)).astype(BF16)
                fs[q, cols, :] = dot_tn(weighted, cv[span, 1024:1152])
            total = fs[1, cols, :] + pair_rows(tt[1, 127:128, :], j) * fs[0, cols, :]
            e_out[j] = (fs[2, cols, :] + pair_rows(tt[2, 127:128, :], j) * total).astype(BF16)

        def go():
            for j in (2 * tile, 2 * tile + 1):
                peer = (y * NZ + j, hd)
                push_if(z != j, e_out.at[j], e_in.at[z], s_send.at[0, j], s_recv.at[0, z], peer)
                push_if(z != j, d_out, d_in.at[z], s_send.at[1, j], s_recv.at[1, z], peer)

        pending.append(go)

    def inner(q, part_of):
        span = slice(q * 128, (q + 1) * 128)
        if part_of == 0:
            scores[...] = jnp.where(row_id >= lane_id, dot_nt(cv[span, 1152:1280], cv[span, 1024:1152]), 0.0)
        table = tt[q]
        for j in (2 * part_of, 2 * part_of + 1):
            cols = slice(j * 128, (j + 1) * 128)
            v = cv[span, cols].astype(F32)
            stepped = v * pair_cols(table, 32, j)
            values = jnp.concatenate(
                [jnp.where(first_half, stepped, 0.0), jnp.where(first_half, 0.0, stepped)], axis=0
            ).astype(BF16)
            weights = []
            for h in (2 * j, 2 * j + 1):
                gap = jnp.minimum(table[:, h : h + 1] - ct[q, h : h + 1, :], 0.0)
                weights.append((scores[...] * jnp.exp(gap)).astype(BF16))
            within = jnp.dot(jnp.concatenate(weights, axis=1), values, preferred_element_type=F32)
            skip = jnp.where(first_half[:1], d_skip[:, 2 * j : 2 * j + 1], d_skip[:, 2 * j + 1 : 2 * j + 2])
            ybuf[span, cols] = within + skip * v

    def ends():
        e_in[z] = e_out[z]

    lane_row = lax.broadcasted_iota(jnp.int32, (1, 128), 1)

    def pick(row, lane):
        return jnp.sum(jnp.where(lane_row == lane, row, 0.0), axis=1, keepdims=True)

    def factor(pair):
        return jnp.where(upper_rows[:, :1], jnp.exp(pair[0]), jnp.exp(pair[1]))

    before = []

    def prefix():
        for k in range(1, NZ):
            source = lax.rem(z + NZ - k, NZ)
            arrived(e_in.at[source], s_recv.at[0, source])
            arrived(d_in.at[source], s_recv.at[1, source])
        running = jnp.zeros((128, 128), F32)
        gone = (jnp.zeros((1, 1), F32), jnp.zeros((1, 1), F32))
        for k in range(NZ):
            pre[k] = running
            before.append(gone)
            row = d_in[k, :1, :]
            pair = (pick(row, 2 * z), pick(row, 2 * z + 1))
            running = factor(pair) * running + e_in[k].astype(F32)
            gone = (gone[0] + pair[0], gone[1] + pair[1])
        row_out[...] = running.astype(BF16)
        rowd_out[...] = jnp.broadcast_to(jnp.where(lane_row == 0, gone[0], gone[1]), (8, 128))
        row_in[y] = running.astype(BF16)
        rowd_in[y] = jnp.broadcast_to(jnp.where(lane_row == 0, gone[0], gone[1]), (8, 128))

        def go():
            for k in range(1, NY):
                push(row_out, row_in.at[y], r_send.at[0, k], r_recv.at[0, k], y_peers[k - 1])
                push(rowd_out, rowd_in.at[y], r_send.at[1, k], r_recv.at[1, k], y_peers[k - 1])

        pending.append(go)

    def back():
        for k in range(1, NY):
            source = lax.rem(y + NY - k, NY)
            arrived(row_in.at[source], r_recv.at[0, k])
            arrived(rowd_in.at[source], r_recv.at[1, k])
        entering = jnp.zeros((128, 128), F32)
        for k in range(NY):
            row = rowd_in[k, :1, :]
            moved = factor((row[:, 0:1], row[:, 1:2])) * entering + row_in[k].astype(F32)
            entering = jnp.where(k < y, moved, entering)
        for k in range(NZ):
            back_out[k] = (factor(before[k]) * entering + pre[k]).astype(BF16)
        sin[z] = back_out[z]

        def go():
            for k in (4, 3, 5, 2, 6, 1, 7):
                peer = lax.rem(z + k, NZ)
                push(back_out.at[peer], sin.at[z], b_send.at[k], b_recv.at[k], z_peers[k - 1])

        pending.append(go)

    def carry():
        for k in range(1, NZ):
            arrived(sin.at[lax.rem(z + NZ - k, NZ)], b_recv.at[k])
        for j in range(8):
            cols = slice(j * 128, (j + 1) * 128)
            entering = sin[j].astype(F32)
            for q in range(CHUNKS):
                span = slice(q * 128, (q + 1) * 128)
                across = dot_nt(cv[span, 1152:1280], entering.astype(BF16))
                ybuf[span, cols] += pair_cols(tt[q], 48, j) * across
                if q < CHUNKS - 1:
                    entering = pair_rows(tt[q, 127:128, :], j) * entering + fs[q, cols, :]

    squares = [jnp.zeros((ROWS, 1), F32)]

    def gate(tile):
        cols = slice(tile * 256, (tile + 1) * 256)
        arrived_if(away, gs.at[0, tile], c_recv.at[6 + tile])
        gated = ybuf[:, cols] * silu(gs[0, tile].astype(F32))
        ybuf[:, cols] = gated
        squares[0] = squares[0] + jnp.sum(gated * gated, axis=1, keepdims=True)

    steps = {
        "begin": begin, "ring": ring, "tinh": tok_in_home, "tin": tok_in_away, "tr": tok_relay, "ta": tok_far, "norm": norm, "mats": mats,
        "dt": dt, "gmats": gmats, "chan": chan, "prep": prep, "conv": conv, "state": end_states, "inner": inner,
        "ends": ends, "prefix": prefix, "back": back, "carry": carry, "gate": gate,
    }
    for step in PLAN:
        later, pending[:] = list(pending), []
        for go in later:
            go()
        steps[step[0]](*step[1:])
    for go in pending:
        go()
    scale = lax.rsqrt(squares[0] / GC + EPS)

    def norm_tile(i, carry):
        cols = pl.ds(pl.multiple_of(i * 128, 128), 128)
        no[:, cols] = (ybuf[:, cols] * scale * gate_gain[:, cols]).astype(BF16)
        return carry

    lax.fori_loop(0, 8, norm_tile, 0)
    wo_load.wait()

    def term(dx, core, into, rows=slice(None)):
        cols = pl.ds(pl.multiple_of(head_of(dx, core) * DB, DB), DB)
        into[...] = jnp.dot(no[rows, :], wo[:, cols], preferred_element_type=F32).astype(into.dtype)

    top, low = half

    def to_sibling(r):
        term(r, 1 - c, sib_out.at[r])

    def keep(r):
        term(r, c, part.at[r])

    def send_sibling(r):
        push(sib_out.at[r], sib_in.at[r], o_send.at[r], o_recv.at[r], sibling)

    def chip_sum(r, rows):
        return part[r, rows, :] + sib_in[r, rows, :].astype(F32)

    for k, rows in enumerate(half):
        term(2, 1 - c, sib_out.at[2, rows, :], rows)
        term(2, c, part.at[2, rows, :], rows)
        push(sib_out.at[2, rows, :], sib_in.at[2, rows, :], o_send.at[2 + 2 * k], o_recv.at[2 + 2 * k], sibling)
    to_sibling(1)
    arrived(sib_in.at[2, top, :], o_recv.at[2])
    far_out[top, :] = chip_sum(2, top).astype(BF16)
    arrived(sib_in.at[2, low, :], o_recv.at[4])
    far_out[low, :] = chip_sum(2, low).astype(BF16)
    push(far_out.at[top, :], far_in.at[0], x_send.at[0], x_recv.at[0], plus)
    send_sibling(1)
    to_sibling(3)
    push(far_out.at[low, :], far_in.at[1], x_send.at[1], x_recv.at[1], minus)
    keep(1)
    send_sibling(3)
    keep(3)
    arrived(sib_in.at[1], o_recv.at[1])
    near_out[0, low, :] = chip_sum(1, low).astype(BF16)
    arrived(sib_in.at[3], o_recv.at[3])
    near_out[1, top, :] = chip_sum(3, top).astype(BF16)
    push(near_out.at[0, low, :], near_in.at[0, low, :], x_send.at[2], x_recv.at[2], plus)
    to_sibling(0)
    push(near_out.at[1, top, :], near_in.at[1, top, :], x_send.at[3], x_recv.at[3], minus)
    keep(0)
    send_sibling(0)
    arrived(far_in.at[0], x_recv.at[0])
    near_out[0, top, :] = (chip_sum(1, top) + far_in[0].astype(F32)).astype(BF16)
    push(near_out.at[0, top, :], near_in.at[0, top, :], x_send.at[4], x_recv.at[4], plus)
    arrived(far_in.at[1], x_recv.at[1])
    near_out[1, low, :] = (chip_sum(3, low) + far_in[1].astype(F32)).astype(BF16)
    push(near_out.at[1, low, :], near_in.at[1, low, :], x_send.at[5], x_recv.at[5], minus)
    arrived(sib_in.at[0], o_recv.at[0])
    part[0] = chip_sum(0, slice(None))
    arrived(near_in.at[0, low, :], x_recv.at[2])
    arrived(near_in.at[1, top, :], x_recv.at[3])
    arrived(near_in.at[0, top, :], x_recv.at[4])
    arrived(near_in.at[1, low, :], x_recv.at[5])
    out_ref[...] = (part[0] + near_in[0].astype(F32) + near_in[1].astype(F32)).astype(BF16)
    for copy in sent:
        copy.wait_send()
    for condition, copy in sent_if:
        pl.when(condition)(copy.wait_send)


def body(tokens, norm_gain, w_in, w_dt, dt_bias, a_log, d_skip, conv_w, conv_b, gate_gain, w_out):
    any_space = pl.BlockSpec(memory_space=pl.ANY)
    vmem = pl.BlockSpec(memory_space=pltpu.VMEM)
    dma = pltpu.SemaphoreType.DMA

    def buf(*shape, dtype=BF16):
        return pltpu.VMEM(shape, dtype)

    scratch = [
        buf(NX, ROWS, 2 * DB), buf(ROWS, 4096), buf(4096, CC), buf(4096, G1), buf(4096, G2),
        buf(NH, 4096), buf(GC, 4096), buf(2, 5, ROWS, 256), buf(2, 4, ROWS, 256),
        buf(2, 1, NH, ROWS, dtype=F32),
        buf(ROWS + 8, CC, dtype=F32), buf(5, 16, 256), buf(5, 16, 256), buf(ROWS, CC), buf(ROWS, GC, dtype=F32),
        buf(CHUNKS, 128, 128, dtype=F32), buf(CHUNKS, NH, 128, dtype=F32), buf(CHUNKS, GC, 128, dtype=F32), buf(128, 128, dtype=F32),
        buf(8, 128, 128), buf(8, 128, dtype=F32), buf(8, 128, 128), buf(8, 8, 128, dtype=F32),
        buf(8, 128, 128, dtype=F32),
        buf(128, 128), buf(8, 128, dtype=F32), buf(NY, 128, 128), buf(NY, 8, 128, dtype=F32),
        buf(8, 128, 128), buf(8, 128, 128),
        buf(ROWS, GC), buf(4, ROWS, DB), buf(4, ROWS, DB), buf(4, ROWS, DB, dtype=F32),
        buf(ROWS, DB), buf(2, ROWS // 2, DB), buf(2, ROWS, DB), buf(2, ROWS, DB),
        dma((6,)), dma((8, 16)), dma((8, 16)), dma((3, 4)), dma((2, 4)), dma((6, 16)), dma((6, 16)),
        dma((16,)), dma((16,)), dma((10,)), dma((10,)), dma((5,)), dma((5,)),
        dma((2, NZ)), dma((2, NZ)), dma((2, NY)), dma((2, NY)), dma((NZ,)), dma((NZ,)),
        dma((5,)), dma((5,)), dma((6,)), dma((6,)),
    ]
    return pl.pallas_call(
        kernel,
        out_shape=jax.ShapeDtypeStruct((ROWS, DB), BF16),
        in_specs=[any_space] * 4 + [vmem] * 7,
        out_specs=vmem,
        scratch_shapes=scratch,
        compiler_params=pltpu.CompilerParams(
            collective_id=0, has_side_effects=True, vmem_limit_bytes=64 * 1024 * 1024 - 65536
        ),
    )(
        tokens, w_in.reshape(SUB, GC + CC), w_dt.T, w_out.reshape(GC, 4096),
        norm_gain.reshape(1, 4096), dt_bias.reshape(1, NH), a_log.reshape(1, NH), d_skip.reshape(1, NH),
        conv_w, conv_b, gate_gain,
    )


def solution(mesh):
    in_specs = (
        P("seq", "head"), P(), P("seq", "head", None), P("seq", "head"), P("head"), P("head"), P("head"),
        P(None, "head", None), P("head", None), P("head", None), P("head", None, None),
    )
    return jax.shard_map(body, mesh=mesh, in_specs=in_specs, out_specs=P("seq", "head"), check_vma=False)
```
